256 devices in a mesh: gx: 32 (over z, y_lo, core), gy: 8 (over y_hi, x).
Axes of the slice: x: 4, y: 4 (y_hi: 2, y_lo: 2; y = y_hi * 2 + y_lo), z: 8, core: 2. Of those that a mesh axis runs over, the one named last changes fastest.
Arguments:
- right_side: float32 [32, 8, 512, 256], P('gx', 'gy'), may hold values from -8 to 8, as said below
- coords: float32 [32, 8, 2, 512], P('gx', 'gy'), may hold values from 0 to 1
- noise: float32 [32, 8, 512], P('gx', 'gy'), may hold values from 0.25 to 1
- intersect: int32 [32, 8, 128], P('gx', 'gy'), may hold values from 0 to 4607, as said below
Outputs:
- solution: float32 [32, 8, 512, 256], P('gx', 'gy')
- residual: float32 [32, 8, 512, 256], P('gx', 'gy')
The draws below stay inside these ranges and needn't reach their ends.
Inputs may be any that keep to these rules, and one draw needn't show every extreme that they name: `right_side`: right-hand sides of order one. `intersect`: each subdomain's list holds 128 distinct indices in increasing order; none names the subdomain itself (block number 4) or a subdomain beyond the first or last one along the second dimension.
All inputs are finite; a program needn't handle non-finite values.
Results may differ from the reference program's by a relative error of at most 0.0003.
Values sent between devices are 32-bit elements; how exact they have to be, the bound alone decides.
A program may use at most 128 MiB of HBM per device.

```python
import math
import jax
import jax.numpy as jnp
from jax import lax

P_SIZE = 512
OV = 128
R = 256
ITERS = 3
CELLS_X = 32
CELLS_Y = 8


def draw_right_side(key, part):
    full_shape = (CELLS_X, CELLS_Y, P_SIZE, R)
    normal_vals = jax.random.normal(key, full_shape, jnp.float32)
    return jnp.clip(normal_vals, -6.0, 6.0)


def draw_intersect(key, part):
    slot_count = 9 * P_SIZE

    def per_cell(cell_id):
        cell_key = jax.random.fold_in(key, cell_id + 7)
        column_id = cell_id % CELLS_Y
        slot_ids = jnp.arange(slot_count, dtype=jnp.int32)
        block_col = slot_ids // P_SIZE % 3
        banned = (slot_ids // P_SIZE == 4) | (block_col == 0) & (column_id == 0) | (block_col == 2) & (column_id == CELLS_Y - 1)
        scores = jax.random.randint(cell_key, (slot_count,), 0, 131072, dtype=jnp.int32) * slot_count + slot_ids
        scores = jnp.where(banned, 1073741824 + slot_ids, scores)
        ranking = jnp.argsort(scores, stable=True)
        return jnp.sort(ranking[:OV]).astype(jnp.int32)
    chosen = jax.vmap(per_cell)(jnp.arange(CELLS_X * CELLS_Y, dtype=jnp.int32))
    return chosen.reshape(CELLS_X, CELLS_Y, OV)


def steps_of(stream_key, shape, shards, smallest, high):
    def one(position, parts):
        heights = jax.random.uniform(jax.random.fold_in(jax.random.fold_in(stream_key, 6), position), (parts,), jnp.float32, smallest / len(shards), high / len(shards))
        return jnp.repeat(jnp.exp(heights), shape[position] // parts).reshape((-1,) + (1,) * (len(shape) - position - 1))

    level = one(*shards[0])
    for cut in shards[1:]:
        level = level * one(*cut)
    return level


def setup_inputs(seed: int = 0) -> dict:
    keys = jax.random.split(jax.random.key(seed), 5)
    right_side = draw_right_side(jax.random.fold_in(keys[4], 71), 0)
    coords = jnp.clip(1.0 * jax.random.uniform(keys[1], (CELLS_X, CELLS_Y, 2, P_SIZE), jnp.float32) ** steps_of(keys[1], (CELLS_X, CELLS_Y, 2, P_SIZE), ((0, 32), (1, 8)), -0.2, 0.2), 0.0, 1.0)
    noise = jnp.clip(jnp.exp(math.log(1.0) - 1.3862944 * jax.random.uniform(keys[2], (CELLS_X, CELLS_Y, P_SIZE), jnp.float32) ** steps_of(keys[2], (CELLS_X, CELLS_Y, P_SIZE), ((0, 32), (1, 8)), -0.2, 0.2)), 0.25, 1.0)
    intersect = draw_intersect(jax.random.fold_in(keys[4], 71), 0)
    return {"right_side": right_side, "coords": coords, "noise": noise, "intersect": intersect}


RANGE_LEN = 0.25
ROOT_THREE = math.sqrt(3.0)
HIGH = lax.Precision.HIGHEST

def kernel_block(rows_pos, cols_pos):
    delta_x = rows_pos[0][:, None] - cols_pos[0][None, :]
    delta_y = rows_pos[1][:, None] - cols_pos[1][None, :]
    distance = jnp.sqrt(delta_x * delta_x + delta_y * delta_y)
    scaled = ROOT_THREE / RANGE_LEN * distance
    clipped = jnp.minimum(distance, 1.0)
    taper_val = jnp.square(jnp.square(1.0 - clipped)) * (4.0 * clipped + 1.0)
    return (1.0 + scaled) * jnp.exp(-scaled) * taper_val

def reference(right_side, coords, noise, intersect):
    cells_x, cells_y, points, rhs_count = right_side.shape
    intersect_len = intersect.shape[2]
    cell_count = cells_x * cells_y
    ext_len = points + intersect_len

    def neighbour(values, cell_row, cell_col, shift_x, shift_y):
        near_row = (cell_row + shift_x) % cells_x
        near_col = cell_col + shift_y
        inside = (near_col >= 0) & (near_col < cells_y)
        fetched = values[near_row, jnp.clip(near_col, 0, cells_y - 1)]
        return jnp.where(inside, fetched, jnp.zeros_like(fetched))

    def operate(vector):

        def per_cell(cell_id):
            cell_row = cell_id // cells_y
            cell_col = cell_id % cells_y
            own_pos = coords[cell_row, cell_col]
            accumulated = noise[cell_row, cell_col][:, None] * vector[cell_row, cell_col]
            for shift_x in (-1, 0, 1):
                for shift_y in (-1, 0, 1):
                    near_info = neighbour(coords, cell_row, cell_col, shift_x, shift_y)
                    near_pos = jnp.stack([near_info[0] + float(shift_x), near_info[1] + float(shift_y)])
                    near_vec = neighbour(vector, cell_row, cell_col, shift_x, shift_y)
                    accumulated = accumulated + jnp.dot(kernel_block(own_pos, near_pos).astype(jnp.float32), near_vec.astype(jnp.float32), precision=HIGH, preferred_element_type=jnp.float32)
            return accumulated
        result = lax.map(per_cell, jnp.arange(cell_count, dtype=jnp.int32))
        return result.reshape(cells_x, cells_y, points, rhs_count)

    def setup_cell(cell_id):
        cell_row = cell_id // cells_y
        cell_col = cell_id % cells_y
        intersect_ids = intersect[cell_row, cell_col]
        block_id = intersect_ids // points
        row_in = intersect_ids % points
        row_of = block_id // 3
        col_of = block_id % 3
        near_row = ((cell_row + row_of - 1) % cells_x).astype(jnp.int32)
        near_col = (cell_col + col_of - 1).astype(jnp.int32)
        pos_x = coords[near_row, near_col, 0, row_in]
        pos_y = coords[near_row, near_col, 1, row_in]
        ov_pos = jnp.stack([pos_x + (row_of - 1).astype(jnp.float32), pos_y + (col_of - 1).astype(jnp.float32)])
        ext_pos = jnp.concatenate([coords[cell_row, cell_col], ov_pos], axis=1)
        ext_noise = jnp.concatenate([noise[cell_row, cell_col], noise[near_row, near_col, row_in]])
        local_matrix = kernel_block(ext_pos, ext_pos) + jnp.diag(ext_noise)
        factor = jnp.linalg.cholesky(local_matrix)
        inv_factor = lax.linalg.triangular_solve(factor, jnp.eye(ext_len, dtype=jnp.float32), left_side=True, lower=True)
        inverse = jnp.dot(inv_factor.T.astype(jnp.float32), inv_factor.astype(jnp.float32), precision=HIGH, preferred_element_type=jnp.float32)
        global_ids = ((near_row * cells_y + near_col) * points + row_in).astype(jnp.int32)
        return (inverse, global_ids)
    inverses, global_ids = lax.map(setup_cell, jnp.arange(cell_count, dtype=jnp.int32))

    def precondition(residue):
        flat_res = residue.reshape(cell_count * points, rhs_count)
        extended = jnp.concatenate([residue.reshape(cell_count, points, rhs_count), flat_res[global_ids]], axis=1)
        solved = jnp.einsum('cij,cjr->cir', inverses, extended, precision=HIGH)
        result = solved[:, :points].reshape(cell_count * points, rhs_count)
        result = result.at[global_ids.reshape(-1)].add(solved[:, points:].reshape(-1, rhs_count))
        return result.reshape(cells_x, cells_y, points, rhs_count)

    def column_sum(first, second):
        return lax.optimization_barrier(jnp.sum(first * second, axis=(0, 1, 2)))
    solution = jnp.zeros_like(right_side)
    residual = right_side
    precond = precondition(residual)
    direction = precond
    inner_now = column_sum(residual, precond)
    for iteration in range(ITERS):
        image_vec = operate(direction)
        step_size = inner_now / column_sum(direction, image_vec)
        solution = solution + step_size * direction
        residual = residual - step_size * image_vec
        if iteration + 1 < ITERS:
            precond = precondition(residual)
            inner_next = column_sum(residual, precond)
            direction = precond + inner_next / inner_now * direction
            inner_now = inner_next
    return (solution, residual)
```

```python
import functools
import math

import jax
import jax.numpy as jnp
from jax import lax
from jax.experimental import pallas as pl
from jax.experimental.pallas import tpu as pltpu
from jax.sharding import PartitionSpec as P

MESH = pl.DeviceIdType.MESH
HIGH = lax.Precision.HIGHEST
F32 = jnp.float32
BF16 = jnp.bfloat16
SCALE = math.sqrt(3.0) / 0.25
LEAST_NOISE = 0.25
NEWTON_STEPS = 7
LANES = 128
NEAR = [(a, b) for a in (-1, 0, 1) for b in (-1, 0, 1) if (a, b) != (0, 0)]
BOTH = (1, -1)


def slot(a, b):
    return (a + 1) * 3 + (b + 1)


def kernel_values(target_x, target_y, source_x, source_y):
    dx = target_x - source_x
    dy = target_y - source_y
    distance = jnp.sqrt(dx * dx + dy * dy)
    scaled = SCALE * distance
    clipped = jnp.minimum(distance, 1.0)
    left = 1.0 - clipped
    square = left * left
    return (1.0 + scaled) * jnp.exp(-scaled) * (square * square * (4.0 * clipped + 1.0))


def halves(value):
    high = value.astype(BF16)
    low = (value - high.astype(F32)).astype(BF16)
    return high, low


def packed(value):
    return jnp.concatenate(halves(value), axis=1)


def bf_dot(left, right):
    return jnp.dot(left, right, preferred_element_type=F32)


def split_dot(high, low, both):
    first = bf_dot(high, both)
    return first[:, :LANES] + first[:, LANES:] + bf_dot(low, both[:, :LANES])


def pick_dot(chosen, both):
    first = bf_dot(chosen, both)
    return first[:, :LANES] + first[:, LANES:]


def full_dot(left, right, dims=((1,), (0,))):
    return lax.dot_general(left, right, (dims, ((), ())), precision=HIGH, preferred_element_type=F32)


def identity(size):
    row = lax.broadcasted_iota(jnp.int32, (size, size), 0)
    return (row == lax.broadcasted_iota(jnp.int32, (size, size), 1)).astype(F32)


def newton_inverse(matrix, result):
    size = matrix.shape[0]
    value = matrix[...]
    largest = jnp.max(jnp.sum(jnp.abs(value), axis=1, keepdims=True), axis=0, keepdims=True)
    alpha = 1.0 / largest
    least = LEAST_NOISE * alpha
    scale = 2.0 / (1.0 + least)
    first = scale * alpha
    result[...] = (2.0 * first) * identity(size) - (first * first) * value

    def step(_, least):
        scale = 2.0 / (1.0 + least)
        current = result[...]
        product = full_dot(matrix[...], current)
        result[...] = scale * full_dot(current, 2.0 * identity(size) - scale * product)
        return 4.0 * least / ((1.0 + least) * (1.0 + least))

    lax.fori_loop(0, NEWTON_STEPS, step, 4.0 * least / ((1.0 + least) * (1.0 + least)))


def body(cfg, info_ref, b_ref, x_ref, r_ref, *scratch):
    ref = dict(zip(cfg["names"], scratch))
    points, ov = cfg["points"], cfg["ov"]
    ext = points + ov
    gx, gy = cfg["gx"], cfg["gy"]
    row, col = lax.axis_index("gx"), lax.axis_index("gy")
    has = {0: None, 1: col < gy - 1, -1: col > 0}
    send_sem, recv_sem = ref["send"], ref["recv"]
    counter = [0]
    pending = {0: [], 1: [], -1: []}
    latest = []

    def guarded(which, action):
        if which == 0:
            action()
        else:
            pl.when(has[which])(action)

    def device(a, b):
        return ((row + a + gx) % gx, (col + b + gy) % gy)

    def copy_to(src, dst, target):
        key = counter[0]
        counter[0] += 1
        return pltpu.make_async_remote_copy(
            src_ref=src, dst_ref=dst, send_sem=send_sem.at[key], recv_sem=recv_sem.at[key],
            device_id=target, device_id_type=MESH)

    def send(src, dst, a, b, guard=None):
        out = b if guard is None else guard
        arrives = -b if guard is None else guard
        desc = copy_to(src, dst, device(a, b))
        guarded(out, desc.start)
        pending[out].append(desc)
        latest.append((out, desc))
        return functools.partial(guarded, arrives, desc.wait_recv)

    def sent(begin, end):
        for out, desc in latest[begin:end]:
            guarded(out, desc.wait_send)
            pending[out][:] = [other for other in pending[out] if other is not desc]

    info_all = ref["info_all"]
    for n in range(9):
        if n != 4:
            info_all[n] = jnp.full(info_all.shape[1:], -1.0, F32)
    info_all[4] = info_ref[...]

    @pl.when((col == 0) | (col == gy - 1))
    def _():
        for name in ("ret", "halo", "part_in", "take_in", "give_in"):
            buf = ref[name]
            flat = math.prod(buf.shape[:-2])
            for n in range(flat):
                index, rest = [], n
                for d in reversed(buf.shape[:-2]):
                    index.append(rest % d)
                    rest //= d
                buf[tuple(reversed(index))] = jnp.zeros(buf.shape[-2:], F32)

    groups = cfg["groups"]

    def partner(axis, stride, count, offset):
        mine = row if axis == "gx" else col
        position = (mine // stride) % count
        other = mine + (((position + offset) % count) - position) * stride
        return (other, col) if axis == "gx" else (row, other)

    barrier = pltpu.get_barrier_semaphore()
    for a, b in NEAR:
        pl.semaphore_signal(barrier, inc=1, device_id=device(a, b), device_id_type=MESH)
    total = len(NEAR)
    for axis, stride, count in groups:
        for offset in range(1, count):
            pl.semaphore_signal(barrier, inc=1, device_id=partner(axis, stride, count, offset), device_id_type=MESH)
            total += 1
    pl.semaphore_wait(barrier, total)

    waits = [send(info_ref, info_all.at[slot(-a, -b)], a, b) for a, b in NEAR]
    for wait in waits:
        wait()

    gather, scatter = ref["gather"], ref["scatter"]
    for e, (a, b) in enumerate(NEAR):
        base = float((3 * (1 - a) + (1 - b)) * points)
        ids = info_all[slot(a, b), :, 0:ov]
        ids_row = ids[3:4, :] - base
        ids_col = jnp.transpose(ids)[:, 3:4] - base
        lane = lax.broadcasted_iota(jnp.int32, (ov, points), 1).astype(F32)
        gather[e * ov:(e + 1) * ov, :] = (lane == ids_col).astype(F32).astype(BF16)
        sub = lax.broadcasted_iota(jnp.int32, (points, ov), 0).astype(F32)
        scatter[:, e * ov:(e + 1) * ov] = (sub == ids_row).astype(F32).astype(BF16)

    def borrow_first(k, h, own):
        asked = pick_dot(gather[...], packed(own))
        out = ref["give_out"]
        for e in range(8):
            a, b = NEAR[e]
            along, across = (a, b) if h == 0 else (b, a)
            out[k, h, slot(along, across)] = asked[e * ov:(e + 1) * ov]
        waits = []
        for step in BOTH:
            a, b = (step, 0) if h == 0 else (0, step)
            s = slot(step, -1)
            waits.append(send(out.at[k, h, s:s + 3], ref["take_in"].at[k, h, (1 - step) // 2], a, b))
        return waits

    def borrow_second(k, h, waits):
        for wait in waits:
            wait()
        out, came = ref["give_out"], ref["take_in"]
        waits = []
        for step in BOTH:
            mix = out.at[k, h, slot(0, step)]
            mix[...] = mix[...] + came[k, h, 0, step + 1] + came[k, h, 1, step + 1]
            a, b = (0, step) if h == 0 else (step, 0)
            waits.append(send(mix, ref["give_in"].at[k, h, (1 - step) // 2], a, b))
        return waits

    def borrow_end(k, h, waits):
        for wait in waits:
            wait()
        came, given = ref["take_in"], ref["give_in"]
        return came[k, h, 0, 1] + came[k, h, 1, 1] + given[k, h, 0] + given[k, h, 1]

    inverse = ref["inverse"]

    def precondition(k, extended, target, hooks=()):
        back, out = ref["ret"], ref["ret_out"]
        both, first = [], []
        for h in range(2):
            pack = ref["pack"].at[h]
            pack[...] = packed(extended[h])
            out[k, h] = split_dot(inverse[0, points:ext], inverse[1, points:ext], pack[...])
            waits = {}
            for a, b in ((0, 1), (0, -1), (1, 0), (-1, 0)):
                waits[a, b] = send(out.at[k, h], back.at[k, h, slot(-a, -b)], a, b)
            first.append(waits)
        for h in range(2):
            target[h] = split_dot(inverse[0, 0:points], inverse[1, 0:points], ref["pack"][h])
        second = []
        for h in range(2):
            waits = []
            for step in BOTH:
                first[h][(0, step) if h == 0 else (step, 0)]()
            for step in BOTH:
                for other in BOTH:
                    if h == 0:
                        waits.append(send(back.at[k, h, slot(0, step)], back.at[k, h, slot(-other, step)],
                                          other, 0, guard=step))
                    else:
                        waits.append(send(back.at[k, h, slot(step, 0)], back.at[k, h, slot(step, -other)],
                                          0, other))
            for step in BOTH:
                waits.append(first[h][(step, 0) if h == 0 else (0, step)])
            second.append(waits)
        for hook in hooks:
            hook()
        for h in range(2):
            for wait in second[h]:
                wait()
            given = jnp.concatenate([packed(back[k, h, slot(a, b)]) for a, b in NEAR], axis=0)
            target[h] = target[h] + pick_dot(scatter[...], given)

    blocks = ref["blocks"]
    noise_col = ref["columns"]

    def operate(k, vector, target, hooks=()):
        halo, out, came = ref["halo"], ref["part_out"], ref["part_in"]
        waits = []
        begin = len(latest)
        for h in range(2):
            waits.append([send(vector.at[h], halo.at[k, h, (1 - step) // 2], *((step, 0) if h == 0 else (0, step)))
                          for step in BOTH])
        end = len(latest)
        noise = noise_col[1, :, 2:3]
        for h in range(2):
            both = packed(vector[h])
            for toward in (0, 1, -1):
                n = slot(toward, 0)
                value = split_dot(blocks[h, n, 0], blocks[h, n, 1], both)
                if toward == 0:
                    target[h] = value + noise * vector[h]
                else:
                    out[k, h, (1 - toward) // 2] = value
        later = []
        for h in range(2):
            for wait in waits[h]:
                wait()
            sources = {-1: packed(halo[k, h, 0]), 1: packed(halo[k, h, 1])}
            sends = []
            for toward in (1, -1, 0):
                value = None
                for source in (-1, 1):
                    n = slot(toward, source)
                    term = split_dot(blocks[h, n, 0], blocks[h, n, 1], sources[source])
                    value = term if value is None else value + term
                if toward == 0:
                    target[h] = target[h] + value
                else:
                    part = out.at[k, h, (1 - toward) // 2]
                    part[...] = part[...] + value
                    a, b = (0, toward) if h == 0 else (toward, 0)
                    sends.append(send(part, came.at[k, h, (1 - toward) // 2], a, b))
            later.append(sends)
            if h < len(hooks):
                hooks[h]()
        for h in range(2):
            for wait in later[h]:
                wait()
            target[h] = target[h] + came[k, h, 0] + came[k, h, 1]
        sent(begin, end)

    sums, gathered = ref["sums"], ref["gathered"]
    offsets = [sum(c for _, _, c in groups[:g]) for g in range(len(groups))]
    open_waits = {}

    def reduce_start(k, stage):
        axis, stride, count = groups[stage]
        waits = []
        for offset in range(1, count):
            desc = copy_to(sums.at[k, stage], gathered.at[k, offsets[stage] + offset],
                           partner(axis, stride, count, offset))
            desc.start()
            pending[0].append(desc)
            waits.append(desc.wait_recv)
        open_waits[k] = waits

    def reduce_end(k, stage):
        for wait in open_waits[k]:
            wait()
        value = sums[k, stage]
        for offset in range(1, groups[stage][2]):
            value = value + gathered[k, offsets[stage] + offset]
        sums[k, stage + 1] = value

    def reduce_open(k, pairs):
        rows = []
        for h in range(2):
            for left, right in pairs(h):
                rows.append(jnp.sum(left * right, axis=0, keepdims=True))
        rows.append(jnp.zeros((4, LANES), F32))
        sums[k, 0] = jnp.concatenate(rows, axis=0)
        reduce_start(k, 0)

    def reduce_next(k, stage):
        reduce_end(k, stage)
        if stage + 1 < len(groups):
            reduce_start(k, stage + 1)

    def reduced(k, h, which):
        return sums[k, len(groups), 2 * h + which:2 * h + which + 1, :]

    def half(h):
        return slice(h * LANES, (h + 1) * LANES)

    be, w0, n0, w1 = ref["be"], ref["w0"], ref["n0"], ref["w1"]
    z0, m0, m1, z1, n1 = ref["z0"], ref["m0"], ref["m1"], ref["z1"], ref["n1"]
    own = slice(0, points)
    waits = [borrow_first(0, h, b_ref[:, half(h)]) for h in range(2)]

    columns = ref["columns"]
    for b in (-1, 0, 1):
        columns[b + 1] = jnp.transpose(info_all[slot(0, b)])
    ids = info_all[4, 3:4, 0:ov]
    picked = jnp.zeros((8, ov), F32)
    sub = lax.broadcasted_iota(jnp.int32, (points, ov), 0).astype(F32)
    line = lax.broadcasted_iota(jnp.int32, (8, points), 0)
    for a, b in NEAR:
        chosen = (sub == ids - float(slot(a, b) * points)).astype(F32)
        shift = jnp.where(line == 0, float(a), jnp.where(line == 1, float(b), 0.0))
        picked = picked + full_dot(info_all[slot(a, b)] + shift, chosen)
    wide = ref["wide"]
    wide[:, own] = info_all[4]
    wide[:, points:ext] = picked
    tall = ref["tall"]
    tall[...] = jnp.transpose(wide[...])
    matrix = ref["matrix"]

    def ext_rows(c, carry):
        rows = pl.ds(pl.multiple_of(c * LANES, LANES), LANES)
        value = kernel_values(tall[rows, 0:1], tall[rows, 1:2], wide[0:1, :], wide[1:2, :])
        at = lax.broadcasted_iota(jnp.int32, (LANES, ext), 0) + c * LANES
        diag = at == lax.broadcasted_iota(jnp.int32, (LANES, ext), 1)
        matrix[rows, :] = value + jnp.where(diag, wide[2:3, :], 0.0)
        return carry

    lax.fori_loop(0, ext // LANES, ext_rows, 0)

    def block_rows(c, carry):
        rows = pl.ds(pl.multiple_of(c * LANES, LANES), LANES)
        for b in (-1, 0, 1):
            for a in (-1, 0, 1):
                source = info_all[slot(a, 0)]
                value = kernel_values(columns[b + 1, rows, 0:1], columns[b + 1, rows, 1:2],
                                      source[0:1, :] + float(a), source[1:2, :] - float(b))
                high, low = halves(value)
                blocks[0, slot(b, a), 0, rows, :] = high
                blocks[0, slot(b, a), 1, rows, :] = low
                high, low = halves(jnp.transpose(value))
                blocks[1, slot(a, b), 0, :, rows] = high
                blocks[1, slot(a, b), 1, :, rows] = low
        return carry

    waits = [borrow_second(0, h, waits[h]) for h in range(2)]
    lax.fori_loop(0, points // LANES, block_rows, 0)

    full = ref["full"]
    at = 0
    for size in cfg["leaves"]:
        now = slice(at, at + size)
        before = slice(0, at)
        leaf, leaf_inverse = ref["leaf"].at[0:size, 0:size], ref["leaf_inverse"].at[0:size, 0:size]
        if at == 0:
            leaf[...] = matrix[now, now]
            newton_inverse(leaf, leaf_inverse)
        else:
            cross = matrix[before, now]
            reach = ref["reach"].at[0:at, 0:size]
            reach[...] = full_dot(full[before, before], cross)
            leaf[...] = matrix[now, now] - full_dot(matrix[now, before], reach[...])
            newton_inverse(leaf, leaf_inverse)
            moved = full_dot(reach[...], leaf_inverse[...])
            full[before, before] = full[before, before] + full_dot(moved, reach[...], ((1,), (1,)))
            full[before, now] = -moved
            full[now, before] = -full_dot(leaf_inverse[...], reach[...], ((1,), (1,)))
        full[now, now] = leaf_inverse[...]
        at += size
    high, low = halves(full[...])
    inverse[0] = high
    inverse[1] = low

    for h in range(2):
        be[h, own] = b_ref[:, half(h)]
        be[h, points:ext] = borrow_end(0, h, waits[h])

    precondition(0, be, z0)
    operate(0, z0, w0.at[:, own])
    reduce_open(0, lambda h: ((be[h, own], z0[h]), (z0[h], w0[h, own])))

    def borrow(k, vector, hook):
        waits = [borrow_first(k, h, vector[h, own]) for h in range(2)]
        waits = [borrow_second(k, h, waits[h]) for h in range(2)]
        hook()
        for h in range(2):
            vector[h, points:ext] = borrow_end(k, h, waits[h])

    borrow(1, w0, lambda: reduce_next(0, 0))
    precondition(1, w0, m0, [lambda: reduce_next(0, 1)])
    operate(1, m0, n0.at[:, own], [lambda: reduce_next(0, 2)])

    for h in range(2):
        alpha = reduced(0, h, 0) / reduced(0, h, 1)
        z1[h] = z0[h] - alpha * m0[h]
        w1[h, own] = w0[h, own] - alpha * n0[h, own]
        be[h, own] = be[h, own] - alpha * w0[h, own]
    reduce_open(1, lambda h: ((be[h, own], z1[h]), (z1[h], w1[h, own])))
    borrow(2, n0, lambda: reduce_next(1, 0))
    for h in range(2):
        alpha = reduced(0, h, 0) / reduced(0, h, 1)
        w1[h, points:ext] = w0[h, points:ext] - alpha * n0[h, points:ext]
    precondition(2, w1, m1, [lambda: reduce_next(1, 1)])
    operate(2, m1, n1, [lambda: reduce_next(1, 2)])

    def steps(h):
        gamma0, delta0 = reduced(0, h, 0), reduced(0, h, 1)
        gamma1, delta1 = reduced(1, h, 0), reduced(1, h, 1)
        alpha0 = gamma0 / delta0
        beta1 = gamma1 / gamma0
        alpha1 = gamma1 / (delta1 - beta1 * gamma1 / alpha0)
        return alpha0, beta1, alpha1, gamma1

    for h in range(2):
        alpha0, beta1, alpha1, _ = steps(h)
        direction = z1[h] + beta1 * z0[h]
        image = w1[h, own] + beta1 * w0[h, own]
        x_ref[:, half(h)] = alpha0 * z0[h] + alpha1 * direction
        be[h, own] = be[h, own] - alpha1 * image
        z1[h] = z1[h] - alpha1 * (m1[h] + beta1 * m0[h])
        w1[h, own] = w1[h, own] - alpha1 * (n1[h] + beta1 * n0[h, own])
        z0[h] = direction
        w0[h, own] = image
    reduce_open(2, lambda h: ((be[h, own], z1[h]), (z1[h], w1[h, own])))
    for stage in range(len(groups)):
        reduce_next(2, stage)
    for h in range(2):
        _, _, alpha1, gamma1 = steps(h)
        gamma2, delta2 = reduced(2, h, 0), reduced(2, h, 1)
        beta2 = gamma2 / gamma1
        alpha2 = gamma2 / (delta2 - beta2 * gamma2 / alpha1)
        x_ref[:, half(h)] = x_ref[:, half(h)] + alpha2 * (z1[h] + beta2 * z0[h])
        r_ref[:, half(h)] = be[h, own] - alpha2 * (w1[h, own] + beta2 * w0[h, own])

    for which in (0, 1, -1):
        def drain(descs=pending[which]):
            for desc in descs:
                desc.wait_send()
        guarded(which, drain)
    assert counter[0] <= cfg["copies"], counter[0]


def make(gx, gy, points, ov, rhs):
    ext = points + ov
    inner = 4 if gx % 4 == 0 and gx > 4 else 2
    groups = (("gy", 1, gy), ("gx", 1, inner), ("gx", inner, gx // inner))
    copies = 8 + 3 * (16 + 8 + 8) + 3 * sum(c - 1 for _, _, c in groups)
    stages = len(groups)
    half = (2, points, LANES)
    tall = (2, ext, LANES)
    shapes = {
        "send": pltpu.SemaphoreType.DMA((copies,)),
        "recv": pltpu.SemaphoreType.DMA((copies,)),
        "info_all": ((9, 8, points), F32),
        "gather": ((8 * ov, points), BF16),
        "scatter": ((points, 8 * ov), BF16),
        "ret": ((3, 2, 9, ov, LANES), F32),
        "ret_out": ((3, 2, ov, LANES), F32),
        "halo": ((3, 2, 2, points, LANES), F32),
        "part_out": ((3, 2, 2, points, LANES), F32),
        "part_in": ((3, 2, 2, points, LANES), F32),
        "give_out": ((3, 2, 9, ov, LANES), F32),
        "take_in": ((3, 2, 2, 3, ov, LANES), F32),
        "give_in": ((3, 2, 2, ov, LANES), F32),
        "pack": ((2, ext, 2 * LANES), BF16),
        "inverse": ((2, ext, ext), BF16),
        "blocks": ((2, 9, 2, points, points), BF16),
        "columns": ((3, points, 8), F32),
        "wide": ((8, ext), F32),
        "tall": ((ext, 8), F32),
        "matrix": ((ext, ext), F32),
        "full": ((ext, ext), F32),
        "leaf": ((256, 256), F32),
        "leaf_inverse": ((256, 256), F32),
        "reach": ((points, 256), F32),
        "sums": ((3, stages + 1, 8, LANES), F32),
        "gathered": ((3, sum(c for _, _, c in groups), 8, LANES), F32),
        "be": (tall, F32), "w0": (tall, F32), "n0": (tall, F32), "w1": (tall, F32),
        "z0": (half, F32), "m0": (half, F32), "m1": (half, F32), "z1": (half, F32), "n1": (half, F32),
    }
    cfg = {"names": tuple(shapes), "points": points, "ov": ov, "gx": gx, "gy": gy, "groups": groups,
           "copies": copies, "leaves": (256,) * (points // 256) + (ov,)}
    scratch = [pltpu.VMEM(*v) if isinstance(v, tuple) else v for v in shapes.values()]
    whole = pl.BlockSpec(memory_space=pltpu.VMEM)
    call = pl.pallas_call(
        functools.partial(body, cfg),
        out_shape=(jax.ShapeDtypeStruct((points, rhs), F32),) * 2,
        in_specs=[whole, whole],
        out_specs=(whole, whole),
        scratch_shapes=scratch,
        compiler_params=pltpu.CompilerParams(
            collective_id=0, has_side_effects=True, vmem_limit_bytes=67043328),
    )

    def shards(right_side, coords, noise, intersect):
        ids = jnp.pad(intersect.reshape(1, ov).astype(F32), ((0, 0), (0, points - ov)))
        info = jnp.concatenate(
            [coords.reshape(2, points), noise.reshape(1, points), ids, jnp.zeros((4, points), F32)], axis=0)
        x, r = call(info, right_side.reshape(points, rhs))
        return x.reshape(right_side.shape), r.reshape(right_side.shape)

    return shards


def solution(mesh):
    gx, gy = mesh.shape["gx"], mesh.shape["gy"]

    def run(right_side, coords, noise, intersect):
        points, rhs = right_side.shape[2:]
        spec4, spec3 = P("gx", "gy", None, None), P("gx", "gy", None)
        return jax.shard_map(
            make(gx, gy, points, intersect.shape[2], rhs), mesh=mesh,
            in_specs=(spec4, spec4, spec3, spec3), out_specs=(spec4, spec4), check_vma=False,
        )(right_side, coords, noise, intersect)

    return run
```

```python
import functools
import math

import jax
import jax.numpy as jnp
from jax import lax
from jax.experimental import pallas as pl
from jax.experimental.pallas import tpu as pltpu
from jax.sharding import PartitionSpec as P

MESH = pl.DeviceIdType.MESH
HIGH = lax.Precision.HIGHEST
F32 = jnp.float32
BF16 = jnp.bfloat16
SCALE = math.sqrt(3.0) / 0.25
LEAST_NOISE = 0.25
NEWTON_STEPS = 7
LANES = 128
NEAR = [(a, b) for a in (-1, 0, 1) for b in (-1, 0, 1) if (a, b) != (0, 0)]
BOTH = (1, -1)


def slot(a, b):
    return (a + 1) * 3 + (b + 1)


def kernel_values(target_x, target_y, source_x, source_y):
    dx = target_x - source_x
    dy = target_y - source_y
    distance = jnp.sqrt(dx * dx + dy * dy)
    scaled = SCALE * distance
    clipped = jnp.minimum(distance, 1.0)
    left = 1.0 - clipped
    square = left * left
    return (1.0 + scaled) * jnp.exp(-scaled) * (square * square * (4.0 * clipped + 1.0))


def halves(value):
    high = value.astype(BF16)
    low = (value - high.astype(F32)).astype(BF16)
    return high, low


def packed(value):
    return jnp.concatenate(halves(value), axis=1)


def bf_dot(left, right):
    return jnp.dot(left, right, preferred_element_type=F32)


def split_dot(high, low, both):
    first = bf_dot(high, both)
    return first[:, :LANES] + first[:, LANES:] + bf_dot(low, both[:, :LANES])


def pick_dot(chosen, both):
    first = bf_dot(chosen, both)
    return first[:, :LANES] + first[:, LANES:]


def three_dot(left, right):
    (left_high, left_low), (right_high, right_low) = halves(left), halves(right)
    return bf_dot(left_high, right_high) + bf_dot(left_high, right_low) + bf_dot(left_low, right_high)


def full_dot(left, right, dims=((1,), (0,))):
    return lax.dot_general(left, right, (dims, ((), ())), precision=HIGH, preferred_element_type=F32)


def identity(size):
    row = lax.broadcasted_iota(jnp.int32, (size, size), 0)
    return (row == lax.broadcasted_iota(jnp.int32, (size, size), 1)).astype(F32)


def newton_inverse(matrix, result):
    size = matrix.shape[0]
    value = matrix[...]
    largest = jnp.max(jnp.sum(jnp.abs(value), axis=1, keepdims=True), axis=0, keepdims=True)
    alpha = 1.0 / largest
    least = LEAST_NOISE * alpha
    scale = 2.0 / (1.0 + least)
    first = scale * alpha
    result[...] = (2.0 * first) * identity(size) - (first * first) * value

    def step(dot, least):
        scale = 2.0 / (1.0 + least)
        current = result[...]
        product = dot(matrix[...], current)
        result[...] = scale * dot(current, 2.0 * identity(size) - scale * product)
        return 4.0 * least / ((1.0 + least) * (1.0 + least))

    least = lax.fori_loop(0, NEWTON_STEPS - 1, lambda _, least: step(three_dot, least),
                          4.0 * least / ((1.0 + least) * (1.0 + least)))
    step(full_dot, least)


def body(cfg, info_ref, b_ref, x_ref, r_ref, *scratch):
    ref = dict(zip(cfg["names"], scratch))
    points, ov = cfg["points"], cfg["ov"]
    ext = points + ov
    gx, gy = cfg["gx"], cfg["gy"]
    seat, col = lax.axis_index("gx"), lax.axis_index("gy")
    mid = gy // 2

    def host(r, c):
        return (r + (c // mid) * (2 - 4 * ((r // 2) % 2)), c)

    row, _ = host(seat, col)
    traded = col >= mid
    has = {0: None, 1: col < gy - 1, -1: col > 0, "traded": traded}
    send_sem, recv_sem = ref["send"], ref["recv"]
    counter = [0]
    pending = {0: [], 1: [], -1: [], "traded": []}
    latest = []

    def guarded(which, action):
        if which == 0:
            action()
        else:
            pl.when(has[which])(action)

    def device(a, b):
        return host((row + a + gx) % gx, (col + b + gy) % gy)

    def heir(a, b):
        return host((seat + a + gx) % gx, (col + b + gy) % gy)

    def holder(a, b):
        return ((row + a + gx) % gx, (col + b + gy) % gy)

    mate = (seat + 2 - 4 * ((seat // 2) % 2), col)

    def copy_to(src, dst, target):
        key = counter[0]
        counter[0] += 1
        return pltpu.make_async_remote_copy(
            src_ref=src, dst_ref=dst, send_sem=send_sem.at[key], recv_sem=recv_sem.at[key],
            device_id=target, device_id_type=MESH)

    def send(src, dst, a, b, guard=None, target=None):
        out = b if guard is None else guard
        arrives = -b if guard is None else guard
        desc = copy_to(src, dst, device(a, b) if target is None else target)
        guarded(out, desc.start)
        pending[out].append(desc)
        latest.append((out, desc))
        return functools.partial(guarded, arrives, desc.wait_recv)

    def sent(begin, end):
        for out, desc in latest[begin:end]:
            guarded(out, desc.wait_send)
            pending[out][:] = [other for other in pending[out] if other is not desc]

    info_all = ref["info_all"]
    for n in range(9):
        if n != 4:
            info_all[n] = jnp.full(info_all.shape[1:], -1.0, F32)

    @pl.when(col < mid)
    def _():
        info_all[4] = info_ref[...]

    @pl.when((col == 0) | (col == gy - 1))
    def _():
        for name in ("ret", "halo", "part_in", "take_in", "give_in"):
            buf = ref[name]
            flat = math.prod(buf.shape[:-2])
            for n in range(flat):
                index, rest = [], n
                for d in reversed(buf.shape[:-2]):
                    index.append(rest % d)
                    rest //= d
                buf[tuple(reversed(index))] = jnp.zeros(buf.shape[-2:], F32)

    groups = cfg["groups"]

    def partner(axis, stride, count, offset):
        mine = seat if axis == "gx" else col
        position = (mine // stride) % count
        other = mine + (((position + offset) % count) - position) * stride
        return (other, col) if axis == "gx" else (seat, other)

    barrier = pltpu.get_barrier_semaphore()
    for a, b in NEAR:
        for whom in (device, heir, holder):
            pl.semaphore_signal(barrier, inc=1, device_id=whom(a, b), device_id_type=MESH)
    pl.semaphore_signal(barrier, inc=1, device_id=mate, device_id_type=MESH)
    total = 3 * len(NEAR) + 1
    for axis, stride, count in groups:
        for offset in range(1, count):
            pl.semaphore_signal(barrier, inc=1, device_id=partner(axis, stride, count, offset), device_id_type=MESH)
            total += 1
    pl.semaphore_wait(barrier, total)

    waits = [send(info_ref, info_all.at[slot(-a, -b)], a, b, target=heir(a, b)) for a, b in NEAR]
    waits.append(send(info_ref, info_all.at[4], 0, 0, guard="traded", target=mate))
    be = ref["be"]
    own = slice(0, points)

    def half(h):
        return slice(h * LANES, (h + 1) * LANES)

    came_right = [send(b_ref.at[:, half(h)], be.at[h, own], 0, 0, guard="traded", target=mate) for h in range(2)]

    @pl.when(col < mid)
    def _():
        for h in range(2):
            be[h, own] = b_ref[:, half(h)]

    for wait in waits:
        wait()

    gather, scatter = ref["gather"], ref["scatter"]
    for e, (a, b) in enumerate(NEAR):
        base = float((3 * (1 - a) + (1 - b)) * points)
        ids = info_all[slot(a, b), :, 0:ov]
        ids_row = ids[3:4, :] - base
        ids_col = jnp.transpose(ids)[:, 3:4] - base
        lane = lax.broadcasted_iota(jnp.int32, (ov, points), 1).astype(F32)
        gather[e * ov:(e + 1) * ov, :] = (lane == ids_col).astype(F32).astype(BF16)
        sub = lax.broadcasted_iota(jnp.int32, (points, ov), 0).astype(F32)
        scatter[:, e * ov:(e + 1) * ov] = (sub == ids_row).astype(F32).astype(BF16)

    def borrow_first(k, h, own):
        asked = pick_dot(gather[...], packed(own))
        out = ref["give_out"]
        for e in range(8):
            a, b = NEAR[e]
            along, across = (a, b) if h == 0 else (b, a)
            out[k, h, slot(along, across)] = asked[e * ov:(e + 1) * ov]
        waits = []
        for step in BOTH:
            a, b = (step, 0) if h == 0 else (0, step)
            s = slot(step, -1)
            waits.append(send(out.at[k, h, s:s + 3], ref["take_in"].at[k, h, (1 - step) // 2], a, b))
        return waits

    def borrow_second(k, h, waits):
        for wait in waits:
            wait()
        out, came = ref["give_out"], ref["take_in"]
        waits = []
        for step in BOTH:
            mix = out.at[k, h, slot(0, step)]
            mix[...] = mix[...] + came[k, h, 0, step + 1] + came[k, h, 1, step + 1]
            a, b = (0, step) if h == 0 else (step, 0)
            waits.append(send(mix, ref["give_in"].at[k, h, (1 - step) // 2], a, b))
        return waits

    def borrow_end(k, h, waits):
        for wait in waits:
            wait()
        came, given = ref["take_in"], ref["give_in"]
        return came[k, h, 0, 1] + came[k, h, 1, 1] + given[k, h, 0] + given[k, h, 1]

    inverse = ref["inverse"]

    def precondition(k, extended, target, hooks=(), early=None, late=None):
        back, out = ref["ret"], ref["ret_out"]
        both, first = [], []
        for h in range(2):
            pack = ref["pack"].at[h]
            pack[...] = packed(extended[h])
            out[k, h] = split_dot(inverse[0, points:ext], inverse[1, points:ext], pack[...])
            waits = {}
            for a, b in ((0, 1), (0, -1), (1, 0), (-1, 0)):
                waits[a, b] = send(out.at[k, h], back.at[k, h, slot(-a, -b)], a, b)
            first.append(waits)
        for h in range(2):
            target[h] = split_dot(inverse[0, 0:points], inverse[1, 0:points], ref["pack"][h])
        if early is not None:
            early()
        second = []
        for h in range(2):
            waits = []
            for step in BOTH:
                first[h][(0, step) if h == 0 else (step, 0)]()
            for step in BOTH:
                for other in BOTH:
                    if h == 0:
                        waits.append(send(back.at[k, h, slot(0, step)], back.at[k, h, slot(-other, step)],
                                          other, 0, guard=step))
                    else:
                        waits.append(send(back.at[k, h, slot(step, 0)], back.at[k, h, slot(step, -other)],
                                          0, other))
            for step in BOTH:
                waits.append(first[h][(step, 0) if h == 0 else (0, step)])
            second.append(waits)
        for hook in hooks:
            hook()
        if late is not None:
            late()
        for h in range(2):
            for wait in second[h]:
                wait()
            given = jnp.concatenate([packed(back[k, h, slot(a, b)]) for a, b in NEAR], axis=0)
            target[h] = target[h] + pick_dot(scatter[...], given)

    blocks = ref["blocks"]
    noise_col = ref["columns"]

    def operate(k, vector, target, hooks=(), early=None):
        halo, out, came = ref["halo"], ref["part_out"], ref["part_in"]
        waits = []
        begin = len(latest)
        for h in range(2):
            waits.append([send(vector.at[h], halo.at[k, h, (1 - step) // 2], *((step, 0) if h == 0 else (0, step)))
                          for step in BOTH])
        end = len(latest)
        noise = noise_col[1, :, 2:3]
        for h in range(2):
            both = packed(vector[h])
            for toward in (0, 1, -1):
                n = slot(toward, 0)
                value = split_dot(blocks[h, n, 0], blocks[h, n, 1], both)
                if toward == 0:
                    target[h] = value + noise * vector[h]
                else:
                    out[k, h, (1 - toward) // 2] = value
        if early is not None:
            early()
        later = []
        for h in range(2):
            for wait in waits[h]:
                wait()
            sources = {-1: packed(halo[k, h, 0]), 1: packed(halo[k, h, 1])}
            sends = []
            for toward in (1, -1, 0):
                value = None
                for source in (-1, 1):
                    n = slot(toward, source)
                    term = split_dot(blocks[h, n, 0], blocks[h, n, 1], sources[source])
                    value = term if value is None else value + term
                if toward == 0:
                    target[h] = target[h] + value
                else:
                    part = out.at[k, h, (1 - toward) // 2]
                    part[...] = part[...] + value
                    a, b = (0, toward) if h == 0 else (toward, 0)
                    sends.append(send(part, came.at[k, h, (1 - toward) // 2], a, b))
            later.append(sends)
            if h < len(hooks):
                hooks[h]()
        for h in range(2):
            for wait in later[h]:
                wait()
            target[h] = target[h] + came[k, h, 0] + came[k, h, 1]
        sent(begin, end)

    sums, gathered = ref["sums"], ref["gathered"]
    offsets = [sum(c for _, _, c in groups[:g]) for g in range(len(groups))]
    open_waits = {}

    def reduce_start(k, stage):
        axis, stride, count = groups[stage]
        waits = []
        for offset in range(1, count):
            desc = copy_to(sums.at[k, stage], gathered.at[k, offsets[stage] + offset],
                           partner(axis, stride, count, offset))
            desc.start()
            pending[0].append(desc)
            waits.append(desc.wait_recv)
        open_waits[k] = waits

    def reduce_end(k, stage):
        for wait in open_waits[k]:
            wait()
        value = sums[k, stage]
        for offset in range(1, groups[stage][2]):
            value = value + gathered[k, offsets[stage] + offset]
        sums[k, stage + 1] = value

    def reduce_open(k, pairs):
        rows = []
        for h in range(2):
            for left, right in pairs(h):
                rows.append(jnp.sum(left * right, axis=0, keepdims=True))
        rows.append(jnp.zeros((4, LANES), F32))
        sums[k, 0] = jnp.concatenate(rows, axis=0)
        reduce_start(k, 0)

    def reduce_next(k, stage):
        reduce_end(k, stage)
        if stage + 1 < len(groups):
            reduce_start(k, stage + 1)

    def reduced(k, h, which):
        return sums[k, len(groups), 2 * h + which:2 * h + which + 1, :]

    w0, n0, w1 = ref["w0"], ref["n0"], ref["w1"]
    z0, m0, m1, z1, n1 = ref["z0"], ref["m0"], ref["m1"], ref["z1"], ref["n1"]
    columns = ref["columns"]
    for b in (-1, 0, 1):
        columns[b + 1] = jnp.transpose(info_all[slot(0, b)])
    ids = info_all[4, 3:4, 0:ov]
    picked = jnp.zeros((8, ov), F32)
    sub = lax.broadcasted_iota(jnp.int32, (points, ov), 0).astype(F32)
    line = lax.broadcasted_iota(jnp.int32, (8, points), 0)
    for a, b in NEAR:
        chosen = (sub == ids - float(slot(a, b) * points)).astype(F32)
        shift = jnp.where(line == 0, float(a), jnp.where(line == 1, float(b), 0.0))
        picked = picked + full_dot(info_all[slot(a, b)] + shift, chosen)
    wide = ref["wide"]
    wide[:, own] = info_all[4]
    wide[:, points:ext] = picked
    tall = ref["tall"]
    tall[...] = jnp.transpose(wide[...])
    matrix = ref["matrix"]

    def ext_rows(c, carry):
        rows = pl.ds(pl.multiple_of(c * LANES, LANES), LANES)
        value = kernel_values(tall[rows, 0:1], tall[rows, 1:2], wide[0:1, :], wide[1:2, :])
        at = lax.broadcasted_iota(jnp.int32, (LANES, ext), 0) + c * LANES
        diag = at == lax.broadcasted_iota(jnp.int32, (LANES, ext), 1)
        matrix[rows, :] = value + jnp.where(diag, wide[2:3, :], 0.0)
        return carry

    lax.fori_loop(0, ext // LANES, ext_rows, 0)

    def build(pairs):
        def block_rows(c, carry):
            rows = pl.ds(pl.multiple_of(c * LANES, LANES), LANES)
            for b, a in pairs:
                source = info_all[slot(a, 0)]
                value = kernel_values(columns[b + 1, rows, 0:1], columns[b + 1, rows, 1:2],
                                      source[0:1, :] + float(a), source[1:2, :] - float(b))
                high, low = halves(value)
                blocks[0, slot(b, a), 0, rows, :] = high
                blocks[0, slot(b, a), 1, rows, :] = low
                high, low = halves(jnp.transpose(value))
                blocks[1, slot(a, b), 0, :, rows] = high
                blocks[1, slot(a, b), 1, :, rows] = low
            return carry

        lax.fori_loop(0, points // LANES, block_rows, 0)

    for wait in came_right:
        wait()
    waits = [borrow_first(0, h, be[h, own]) for h in range(2)]

    full = ref["full"]
    at = 0
    for size in cfg["leaves"]:
        now = slice(at, at + size)
        before = slice(0, at)
        leaf, leaf_inverse = ref["leaf"].at[0:size, 0:size], ref["leaf_inverse"].at[0:size, 0:size]
        if at == 0:
            leaf[...] = matrix[now, now]
            newton_inverse(leaf, leaf_inverse)
        else:
            cross = matrix[before, now]
            reach = ref["reach"].at[0:at, 0:size]
            reach[...] = full_dot(full[before, before], cross)
            leaf[...] = matrix[now, now] - full_dot(matrix[now, before], reach[...])
            newton_inverse(leaf, leaf_inverse)
            moved = full_dot(reach[...], leaf_inverse[...])
            full[before, before] = full[before, before] + full_dot(moved, reach[...], ((1,), (1,)))
            full[before, now] = -moved
            full[now, before] = -full_dot(leaf_inverse[...], reach[...], ((1,), (1,)))
        if at == 0:
            waits = [borrow_second(0, h, waits[h]) for h in range(2)]
        full[now, now] = leaf_inverse[...]
        at += size
    high, low = halves(full[...])
    inverse[0] = high
    inverse[1] = low

    for h in range(2):
        be[h, points:ext] = borrow_end(0, h, waits[h])

    precondition(0, be, z0, early=lambda: build([(0, 0), (1, 0), (-1, 0)]), late=lambda: build([(0, 1), (0, -1)]))
    operate(0, z0, w0.at[:, own], early=lambda: build([(1, 1), (1, -1), (-1, 1), (-1, -1)]))
    reduce_open(0, lambda h: ((be[h, own], z0[h]), (z0[h], w0[h, own])))

    def borrow(k, vector, hook):
        waits = [borrow_first(k, h, vector[h, own]) for h in range(2)]
        waits = [borrow_second(k, h, waits[h]) for h in range(2)]
        hook()
        for h in range(2):
            vector[h, points:ext] = borrow_end(k, h, waits[h])

    borrow(1, w0, lambda: reduce_next(0, 0))
    precondition(1, w0, m0, [lambda: reduce_next(0, 1)])
    operate(1, m0, n0.at[:, own], [lambda: reduce_next(0, 2)])

    for h in range(2):
        alpha = reduced(0, h, 0) / reduced(0, h, 1)
        z1[h] = z0[h] - alpha * m0[h]
        w1[h, own] = w0[h, own] - alpha * n0[h, own]
        be[h, own] = be[h, own] - alpha * w0[h, own]
    reduce_open(1, lambda h: ((be[h, own], z1[h]), (z1[h], w1[h, own])))
    borrow(2, n0, lambda: reduce_next(1, 0))
    for h in range(2):
        alpha = reduced(0, h, 0) / reduced(0, h, 1)
        w1[h, points:ext] = w0[h, points:ext] - alpha * n0[h, points:ext]
    precondition(2, w1, m1, [lambda: reduce_next(1, 1)])
    operate(2, m1, n1, [lambda: reduce_next(1, 2)])

    def steps(h):
        gamma0, delta0 = reduced(0, h, 0), reduced(0, h, 1)
        gamma1, delta1 = reduced(1, h, 0), reduced(1, h, 1)
        alpha0 = gamma0 / delta0
        beta1 = gamma1 / gamma0
        alpha1 = gamma1 / (delta1 - beta1 * gamma1 / alpha0)
        return alpha0, beta1, alpha1, gamma1

    result, got = ref["result"], ref["got"]

    for h in range(2):
        alpha0, beta1, alpha1, _ = steps(h)
        direction = z1[h] + beta1 * z0[h]
        image = w1[h, own] + beta1 * w0[h, own]
        result[0, h] = alpha0 * z0[h] + alpha1 * direction
        be[h, own] = be[h, own] - alpha1 * image
        z1[h] = z1[h] - alpha1 * (m1[h] + beta1 * m0[h])
        w1[h, own] = w1[h, own] - alpha1 * (n1[h] + beta1 * n0[h, own])
        z0[h] = direction
        w0[h, own] = image
    reduce_open(2, lambda h: ((be[h, own], z1[h]), (z1[h], w1[h, own])))
    for stage in range(len(groups)):
        reduce_next(2, stage)
    home = []
    for h in range(2):
        _, _, alpha1, gamma1 = steps(h)
        gamma2, delta2 = reduced(2, h, 0), reduced(2, h, 1)
        beta2 = gamma2 / gamma1
        alpha2 = gamma2 / (delta2 - beta2 * gamma2 / alpha1)
        result[0, h] = result[0, h] + alpha2 * (z1[h] + beta2 * z0[h])
        home.append(send(result.at[0, h], got.at[0, h], 0, 0, guard="traded", target=mate))
        result[1, h] = be[h, own] - alpha2 * (w1[h, own] + beta2 * w0[h, own])
        home.append(send(result.at[1, h], got.at[1, h], 0, 0, guard="traded", target=mate))

    @pl.when(col < mid)
    def _():
        for h in range(2):
            x_ref[:, half(h)] = result[0, h]
            r_ref[:, half(h)] = result[1, h]

    for n, wait in enumerate(home):
        wait()

        @pl.when(traded)
        def _():
            (x_ref, r_ref)[n % 2][:, half(n // 2)] = got[n % 2, n // 2]

    for which in (0, 1, -1, "traded"):
        def drain(descs=pending[which]):
            for desc in descs:
                desc.wait_send()
        guarded(which, drain)
    assert counter[0] <= cfg["copies"], counter[0]


def make(gx, gy, points, ov, rhs):
    ext = points + ov
    inner = 4 if gx % 4 == 0 and gx > 4 else 2
    groups = (("gy", 1, gy), ("gx", 1, inner), ("gx", inner, gx // inner))
    copies = 8 + 7 + 3 * (16 + 8 + 8) + 3 * sum(c - 1 for _, _, c in groups)
    stages = len(groups)
    half = (2, points, LANES)
    tall = (2, ext, LANES)
    shapes = {
        "send": pltpu.SemaphoreType.DMA((copies,)),
        "recv": pltpu.SemaphoreType.DMA((copies,)),
        "info_all": ((9, 8, points), F32),
        "gather": ((8 * ov, points), BF16),
        "scatter": ((points, 8 * ov), BF16),
        "ret": ((3, 2, 9, ov, LANES), F32),
        "ret_out": ((3, 2, ov, LANES), F32),
        "halo": ((3, 2, 2, points, LANES), F32),
        "part_out": ((3, 2, 2, points, LANES), F32),
        "part_in": ((3, 2, 2, points, LANES), F32),
        "give_out": ((3, 2, 9, ov, LANES), F32),
        "take_in": ((3, 2, 2, 3, ov, LANES), F32),
        "give_in": ((3, 2, 2, ov, LANES), F32),
        "pack": ((2, ext, 2 * LANES), BF16),
        "inverse": ((2, ext, ext), BF16),
        "blocks": ((2, 9, 2, points, points), BF16),
        "columns": ((3, points, 8), F32),
        "wide": ((8, ext), F32),
        "tall": ((ext, 8), F32),
        "matrix": ((ext, ext), F32),
        "full": ((ext, ext), F32),
        "leaf": ((256, 256), F32),
        "leaf_inverse": ((256, 256), F32),
        "reach": ((points, 256), F32),
        "result": ((2, 2, points, LANES), F32),
        "got": ((2, 2, points, LANES), F32),
        "sums": ((3, stages + 1, 8, LANES), F32),
        "gathered": ((3, sum(c for _, _, c in groups), 8, LANES), F32),
        "be": (tall, F32), "w0": (tall, F32), "n0": (tall, F32), "w1": (tall, F32),
        "z0": (half, F32), "m0": (half, F32), "m1": (half, F32), "z1": (half, F32), "n1": (half, F32),
    }
    cfg = {"names": tuple(shapes), "points": points, "ov": ov, "gx": gx, "gy": gy, "groups": groups,
           "copies": copies, "leaves": (256,) * (points // 256) + (ov,)}
    scratch = [pltpu.VMEM(*v) if isinstance(v, tuple) else v for v in shapes.values()]
    whole = pl.BlockSpec(memory_space=pltpu.VMEM)
    call = pl.pallas_call(
        functools.partial(body, cfg),
        out_shape=(jax.ShapeDtypeStruct((points, rhs), F32),) * 2,
        in_specs=[whole, whole],
        out_specs=(whole, whole),
        scratch_shapes=scratch,
        compiler_params=pltpu.CompilerParams(
            collective_id=0, has_side_effects=True, vmem_limit_bytes=67043328),
    )

    def shards(right_side, coords, noise, intersect):
        ids = jnp.pad(intersect.reshape(1, ov).astype(F32), ((0, 0), (0, points - ov)))
        info = jnp.concatenate(
            [coords.reshape(2, points), noise.reshape(1, points), ids, jnp.zeros((4, points), F32)], axis=0)
        x, r = call(info, right_side.reshape(points, rhs))
        return x.reshape(right_side.shape), r.reshape(right_side.shape)

    return shards


def solution(mesh):
    gx, gy = mesh.shape["gx"], mesh.shape["gy"]

    def run(right_side, coords, noise, intersect):
        points, rhs = right_side.shape[2:]
        spec4, spec3 = P("gx", "gy", None, None), P("gx", "gy", None)
        return jax.shard_map(
            make(gx, gy, points, intersect.shape[2], rhs), mesh=mesh,
            in_specs=(spec4, spec4, spec3, spec3), out_specs=(spec4, spec4), check_vma=False,
        )(right_side, coords, noise, intersect)

    return run
```

```python
import functools
import math

import jax
import jax.numpy as jnp
from jax import lax
from jax.experimental import pallas as pl
from jax.experimental.pallas import tpu as pltpu
from jax.sharding import PartitionSpec as P

MESH = pl.DeviceIdType.MESH
HIGH = lax.Precision.HIGHEST
F32 = jnp.float32
BF16 = jnp.bfloat16
SCALE = math.sqrt(3.0) / 0.25
LEAST_NOISE = 0.25
NEWTON_STEPS = 7
LANES = 128
NEAR = [(a, b) for a in (-1, 0, 1) for b in (-1, 0, 1) if (a, b) != (0, 0)]
BOTH = (1, -1)


def slot(a, b):
    return (a + 1) * 3 + (b + 1)


def kernel_values(target_x, target_y, source_x, source_y):
    dx = target_x - source_x
    dy = target_y - source_y
    square = dx * dx + dy * dy
    distance = square * lax.rsqrt(jnp.maximum(square, 1e-30))
    scaled = SCALE * distance
    clipped = jnp.minimum(distance, 1.0)
    left = 1.0 - clipped
    square = left * left
    return (1.0 + scaled) * jnp.exp(-scaled) * (square * square * (4.0 * clipped + 1.0))


def halves(value):
    high = value.astype(BF16)
    low = (value - high.astype(F32)).astype(BF16)
    return high, low


def packed(value):
    return jnp.concatenate(halves(value), axis=1)


def bf_dot(left, right):
    return jnp.dot(left, right, preferred_element_type=F32)


def split_dot(high, low, both):
    first = bf_dot(high, both)
    return first[:, :LANES] + first[:, LANES:] + bf_dot(low, both[:, :LANES])


def pick_dot(chosen, both):
    first = bf_dot(chosen, both)
    return first[:, :LANES] + first[:, LANES:]


def three_dot(left, right):
    (left_high, left_low), (right_high, right_low) = halves(left), halves(right)
    return bf_dot(left_high, right_high) + bf_dot(left_high, right_low) + bf_dot(left_low, right_high)


def full_dot(left, right, dims=((1,), (0,))):
    return lax.dot_general(left, right, (dims, ((), ())), precision=HIGH, preferred_element_type=F32)


def identity(size):
    row = lax.broadcasted_iota(jnp.int32, (size, size), 0)
    return (row == lax.broadcasted_iota(jnp.int32, (size, size), 1)).astype(F32)


def newton_inverse(matrix, result):
    size = matrix.shape[0]
    value = matrix[...]
    largest = jnp.max(jnp.sum(jnp.abs(value), axis=1, keepdims=True), axis=0, keepdims=True)
    alpha = 1.0 / largest
    least = LEAST_NOISE * alpha
    scale = 2.0 / (1.0 + least)
    first = scale * alpha
    result[...] = (2.0 * first) * identity(size) - (first * first) * value

    def step(dot, least):
        scale = 2.0 / (1.0 + least)
        current = result[...]
        product = dot(matrix[...], current)
        result[...] = scale * dot(current, 2.0 * identity(size) - scale * product)
        return 4.0 * least / ((1.0 + least) * (1.0 + least))

    least = lax.fori_loop(0, NEWTON_STEPS - 1, lambda _, least: step(three_dot, least),
                          4.0 * least / ((1.0 + least) * (1.0 + least)))
    step(full_dot, least)


def body(cfg, info_ref, b_ref, x_ref, r_ref, *scratch):
    ref = dict(zip(cfg["names"], scratch))
    points, ov = cfg["points"], cfg["ov"]
    ext = points + ov
    gx, gy = cfg["gx"], cfg["gy"]
    seat, col = lax.axis_index("gx"), lax.axis_index("gy")
    mid = gy // 2

    def trades(r, c):
        return (c // mid + r) % 2

    def host(r, c):
        return (r + trades(r, c) * (2 - 4 * ((r // 2) % 2)), c)

    row, _ = host(seat, col)
    traded, kept = trades(seat, col) == 1, trades(seat, col) == 0
    has = {0: None, 1: col < gy - 1, -1: col > 0, "traded": traded}
    send_sem, recv_sem = ref["send"], ref["recv"]
    counter = [0]
    pending = {0: [], 1: [], -1: [], "traded": []}
    latest = []

    def guarded(which, action):
        if which == 0:
            action()
        else:
            pl.when(has[which])(action)

    def device(a, b):
        return host((row + a + gx) % gx, (col + b + gy) % gy)

    def heir(a, b):
        return host((seat + a + gx) % gx, (col + b + gy) % gy)

    def holder(a, b):
        return ((row + a + gx) % gx, (col + b + gy) % gy)

    mate = (seat + 2 - 4 * ((seat // 2) % 2), col)

    def copy_to(src, dst, target):
        key = counter[0]
        counter[0] += 1
        return pltpu.make_async_remote_copy(
            src_ref=src, dst_ref=dst, send_sem=send_sem.at[key], recv_sem=recv_sem.at[key],
            device_id=target, device_id_type=MESH)

    def send(src, dst, a, b, guard=None, target=None):
        out = b if guard is None else guard
        arrives = -b if guard is None else guard
        desc = copy_to(src, dst, device(a, b) if target is None else target)
        guarded(out, desc.start)
        pending[out].append(desc)
        latest.append((out, desc))
        return functools.partial(guarded, arrives, desc.wait_recv)

    def sent(begin, end):
        for out, desc in latest[begin:end]:
            guarded(out, desc.wait_send)
            pending[out][:] = [other for other in pending[out] if other is not desc]

    info_all = ref["info_all"]
    for n in range(9):
        if n != 4:
            info_all[n] = jnp.full(info_all.shape[1:], -1.0, F32)

    @pl.when(kept)
    def _():
        info_all[4] = info_ref[...]

    @pl.when((col == 0) | (col == gy - 1))
    def _():
        for name in ("ret", "halo", "part_in", "take_in", "give_in"):
            buf = ref[name]
            flat = math.prod(buf.shape[:-2])
            for n in range(flat):
                index, rest = [], n
                for d in reversed(buf.shape[:-2]):
                    index.append(rest % d)
                    rest //= d
                buf[tuple(reversed(index))] = jnp.zeros(buf.shape[-2:], F32)

    groups = cfg["groups"]

    def partner(stride, many, columns_too, offset):
        position = (seat // stride) % many
        ahead = (position + offset % many) % many
        return (seat + (ahead - position) * stride, (col + offset // many) % gy if columns_too > 1 else col)

    barrier = pltpu.get_barrier_semaphore()
    for a, b in NEAR:
        for whom in (device, heir, holder):
            pl.semaphore_signal(barrier, inc=1, device_id=whom(a, b), device_id_type=MESH)
    pl.semaphore_signal(barrier, inc=1, device_id=mate, device_id_type=MESH)
    total = 3 * len(NEAR) + 1
    for group in groups:
        for offset in range(1, group[1] * group[2]):
            pl.semaphore_signal(barrier, inc=1, device_id=partner(*group, offset), device_id_type=MESH)
            total += 1
    pl.semaphore_wait(barrier, total)

    waits = [send(info_ref, info_all.at[slot(-a, -b)], a, b, target=heir(a, b)) for a, b in NEAR]
    waits.append(send(info_ref, info_all.at[4], 0, 0, guard="traded", target=mate))
    be = ref["be"]
    own = slice(0, points)

    def half(h):
        return slice(h * LANES, (h + 1) * LANES)

    came_right = [send(b_ref.at[:, half(h)], be.at[h, own], 0, 0, guard="traded", target=mate) for h in range(2)]

    @pl.when(kept)
    def _():
        for h in range(2):
            be[h, own] = b_ref[:, half(h)]

    for wait in waits:
        wait()

    gather, scatter = ref["gather"], ref["scatter"]

    def chosen_row(ids):
        sub = lax.broadcasted_iota(jnp.int32, (points, ov), 0).astype(F32)
        return (sub == ids).astype(F32).astype(BF16)

    def first_id(a, b):
        return float((3 * (1 - a) + (1 - b)) * points)

    def make_gather():
        for e, (a, b) in enumerate(NEAR):
            ids_col = jnp.transpose(info_all[slot(a, b), :, 0:ov])[:, 3:4] - first_id(a, b)
            lane = lax.broadcasted_iota(jnp.int32, (ov, points), 1).astype(F32)
            gather[e * ov:(e + 1) * ov, :] = (lane == ids_col).astype(F32).astype(BF16)

    def make_scatter():
        for e, (a, b) in enumerate(NEAR):
            scatter[:, e * ov:(e + 1) * ov] = chosen_row(info_all[slot(a, b), 3:4, 0:ov] - first_id(a, b))

    def borrow_first(k, h, own):
        out = ref["give_out"]
        asked = pick_dot(gather[...], packed(own))
        for e in range(8):
            a, b = NEAR[e]
            along, across = (a, b) if h == 0 else (b, a)
            out[k, h, slot(along, across)] = asked[e * ov:(e + 1) * ov]
        waits = []
        for step in BOTH:
            a, b = (step, 0) if h == 0 else (0, step)
            s = slot(step, -1)
            waits.append(send(out.at[k, h, s:s + 3], ref["take_in"].at[k, h, (1 - step) // 2], a, b))
        return waits

    def borrow_second(k, h, waits):
        for wait in waits:
            wait()
        out, came = ref["give_out"], ref["take_in"]
        waits = []
        for step in BOTH:
            mix = out.at[k, h, slot(0, step)]
            mix[...] = mix[...] + came[k, h, 0, step + 1] + came[k, h, 1, step + 1]
            a, b = (0, step) if h == 0 else (step, 0)
            waits.append(send(mix, ref["give_in"].at[k, h, (1 - step) // 2], a, b))
        return waits

    def borrow_end(k, h, waits):
        for wait in waits:
            wait()
        came, given = ref["take_in"], ref["give_in"]
        return came[k, h, 0, 1] + came[k, h, 1, 1] + given[k, h, 0] + given[k, h, 1]

    inverse = ref["inverse"]

    def precondition(k, extended, target, hooks=(), early=None, late=None):
        back, out = ref["ret"], ref["ret_out"]
        both, first = [], []
        for h in range(2):
            pack = ref["pack"].at[h]
            pack[...] = packed(extended[h])
            out[k, h] = split_dot(inverse[0, points:ext], inverse[1, points:ext], pack[...])
            waits = {}
            for a, b in ((0, 1), (0, -1), (1, 0), (-1, 0)):
                waits[a, b] = send(out.at[k, h], back.at[k, h, slot(-a, -b)], a, b)
            first.append(waits)

        def own_rows(h, carry):
            target[h] = split_dot(inverse[0, 0:points], inverse[1, 0:points], ref["pack"][h])
            return carry

        lax.fori_loop(0, 2, own_rows, 0)
        if early is not None:
            early()
        second = []
        for h in range(2):
            waits = []
            for step in BOTH:
                first[h][(0, step) if h == 0 else (step, 0)]()
            for step in BOTH:
                for other in BOTH:
                    if h == 0:
                        waits.append(send(back.at[k, h, slot(0, step)], back.at[k, h, slot(-other, step)],
                                          other, 0, guard=step))
                    else:
                        waits.append(send(back.at[k, h, slot(step, 0)], back.at[k, h, slot(step, -other)],
                                          0, other))
            for step in BOTH:
                waits.append(first[h][(step, 0) if h == 0 else (0, step)])
            second.append(waits)
        for hook in hooks:
            hook()
        if late is not None:
            late()
        for h in range(2):
            for wait in second[h]:
                wait()
            given = jnp.concatenate([packed(back[k, h, slot(a, b)]) for a, b in NEAR], axis=0)
            target[h] = target[h] + pick_dot(scatter[...], given)

    blocks = ref["blocks"]
    noise_col = ref["columns"]

    def operate(k, vector, target, hooks=(), early=None):
        halo, out, came = ref["halo"], ref["part_out"], ref["part_in"]
        waits = []
        begin = len(latest)
        for h in range(2):
            waits.append([send(vector.at[h], halo.at[k, h, (1 - step) // 2], *((step, 0) if h == 0 else (0, step)))
                          for step in BOTH])
        end = len(latest)
        noise = noise_col[1, :, 2:3]
        for h in range(2):
            ref["pack"][h, own] = packed(vector[h])

        def from_here(n, carry):
            h, t = n // 3, n % 3
            out[k, h, t] = split_dot(blocks[h, 7 - 3 * t, 0], blocks[h, 7 - 3 * t, 1], ref["pack"][h, own])
            return carry

        lax.fori_loop(0, 6, from_here, 0)
        if early is not None:
            early()
        def arrived(h, toward):
            value = None
            for source in (-1, 1):
                n = slot(toward, source)
                term = split_dot(blocks[h, n, 0], blocks[h, n, 1], sources[h][source])
                value = term if value is None else value + term
            return value

        later, sources = [], []
        for h in range(2):
            for wait in waits[h]:
                wait()
            sources.append({-1: packed(halo[k, h, 0]), 1: packed(halo[k, h, 1])})
            sends = []
            for toward in BOTH:
                part = out.at[k, h, 1 - toward]
                part[...] = part[...] + arrived(h, toward)
                a, b = (0, toward) if h == 0 else (toward, 0)
                sends.append(send(part, came.at[k, h, (1 - toward) // 2], a, b))
            later.append(sends)
        for h in range(2):
            target[h] = (out[k, h, 1] + noise * vector[h]) + arrived(h, 0)
        for hook in hooks:
            hook()
        for h in range(2):
            for wait in later[h]:
                wait()
            target[h] = target[h] + came[k, h, 0] + came[k, h, 1]
        sent(begin, end)

    sums, gathered = ref["sums"], ref["gathered"]
    counts = [many * columns_too for _, many, columns_too in groups]
    offsets = [sum(counts[:g]) for g in range(len(groups))]
    open_waits = {}

    def reduce_start(k, stage):
        waits = []
        for offset in range(1, counts[stage]):
            desc = copy_to(sums.at[k, stage], gathered.at[k, offsets[stage] + offset],
                           partner(*groups[stage], offset))
            desc.start()
            pending[0].append(desc)
            waits.append(desc.wait_recv)
        open_waits[k] = waits

    def reduce_end(k, stage):
        for wait in open_waits[k]:
            wait()
        value = sums[k, stage]
        for offset in range(1, counts[stage]):
            value = value + gathered[k, offsets[stage] + offset]
        sums[k, stage + 1] = value

    def reduce_open(k, pairs):
        rows = []
        for h in range(2):
            for left, right in pairs(h):
                rows.append(jnp.sum(left * right, axis=0, keepdims=True))
        rows.append(jnp.zeros((4, LANES), F32))
        sums[k, 0] = jnp.concatenate(rows, axis=0)
        reduce_start(k, 0)

    def reduce_next(k, stage):
        reduce_end(k, stage)
        if stage + 1 < len(groups):
            reduce_start(k, stage + 1)

    def reduced(k, h, which):
        return sums[k, len(groups), 2 * h + which:2 * h + which + 1, :]

    w0, n0, w1 = ref["w0"], ref["n0"], ref["w1"]
    z0, m0, m1, z1, n1 = ref["z0"], ref["m0"], ref["m1"], ref["z1"], ref["n1"]
    columns = ref["columns"]
    for b in (-1, 0, 1):
        columns[b + 1] = jnp.transpose(info_all[slot(0, b)])
    ids = info_all[4, 3:4, 0:ov]
    picked = jnp.zeros((32, ov), F32)
    line = lax.broadcasted_iota(jnp.int32, (8, points), 0)
    for a, b in NEAR:
        shift = jnp.where(line == 0, float(a), jnp.where(line == 1, float(b), 0.0))
        value = info_all[slot(a, b)] + shift
        high, middle = halves(value)
        low = (value - high.astype(F32) - middle.astype(F32)).astype(BF16)
        pieces = jnp.concatenate([high.astype(F32), middle.astype(F32), low.astype(F32), jnp.zeros((8, points), F32)])
        picked = picked + bf_dot(pieces.astype(BF16), chosen_row(ids - float(slot(a, b) * points)))
    picked = (picked[0:8] + picked[8:16]) + picked[16:24]
    wide = ref["wide"]
    wide[:, own] = info_all[4]
    wide[:, points:ext] = picked
    tall = ref["tall"]
    tall[...] = jnp.transpose(wide[...])
    matrix = ref["matrix"]

    def ext_rows(c, carry):
        rows = pl.ds(pl.multiple_of(c * LANES, LANES), LANES)
        value = kernel_values(tall[rows, 0:1], tall[rows, 1:2], wide[0:1, :], wide[1:2, :])
        at = lax.broadcasted_iota(jnp.int32, (LANES, ext), 0) + c * LANES
        diag = at == lax.broadcasted_iota(jnp.int32, (LANES, ext), 1)
        matrix[rows, :] = value + jnp.where(diag, wide[2:3, :], 0.0)
        return carry

    lax.fori_loop(0, ext // LANES, ext_rows, 0)

    def build(count, pair):
        def block_rows(n, carry):
            b, a = pair(n // (points // LANES))
            rows = pl.ds(pl.multiple_of(n % (points // LANES) * LANES, LANES), LANES)
            source = info_all[3 * a + 4]
            value = kernel_values(columns[b + 1, rows, 0:1], columns[b + 1, rows, 1:2],
                                  source[0:1, :] + a.astype(F32), source[1:2, :] - b.astype(F32))
            high, low = halves(value)
            blocks[0, slot(b, a), 0, rows, :] = high
            blocks[0, slot(b, a), 1, rows, :] = low
            high, low = halves(jnp.transpose(value))
            blocks[1, slot(a, b), 0, :, rows] = high
            blocks[1, slot(a, b), 1, :, rows] = low
            return carry

        lax.fori_loop(0, count * (points // LANES), block_rows, 0)

    full = ref["full"]
    at = 0
    for size in cfg["leaves"]:
        now = slice(at, at + size)
        before = slice(0, at)
        leaf, leaf_inverse = ref["leaf"].at[0:size, 0:size], ref["leaf_inverse"].at[0:size, 0:size]
        if at == 0:
            leaf[...] = matrix[now, now]
            newton_inverse(leaf, leaf_inverse)
        else:
            cross = matrix[before, now]
            reach = ref["reach"].at[0:at, 0:size]
            reach[...] = full_dot(full[before, before], cross)
            leaf[...] = matrix[now, now] - full_dot(matrix[now, before], reach[...])
            newton_inverse(leaf, leaf_inverse)
            moved = full_dot(reach[...], leaf_inverse[...])
            full[before, before] = full[before, before] + full_dot(moved, reach[...], ((1,), (1,)))
            full[before, now] = -moved
            full[now, before] = -full_dot(leaf_inverse[...], reach[...], ((1,), (1,)))
        if at == 0:
            make_gather()
            for wait in came_right:
                wait()
            waits = [borrow_first(0, h, be[h, own]) for h in range(2)]
        elif at + size == points:
            waits = [borrow_second(0, h, waits[h]) for h in range(2)]
        full[now, now] = leaf_inverse[...]
        at += size
    high, low = halves(full[...])
    inverse[0] = high
    inverse[1] = low

    for h in range(2):
        be[h, points:ext] = borrow_end(0, h, waits[h])

    precondition(0, be, z0, early=lambda: build(3, lambda n: (n - 1, 0 * n)), late=lambda: (make_scatter(), build(2, lambda n: (0 * n, 2 * n - 1))))
    operate(0, z0, w0.at[:, own], early=lambda: build(4, lambda n: (2 * (n // 2) - 1, 2 * (n % 2) - 1)))
    reduce_open(0, lambda h: ((be[h, own], z0[h]), (z0[h], w0[h, own])))

    def borrow(k, vector, hook):
        waits = [borrow_first(k, h, vector[h, own]) for h in range(2)]
        waits = [borrow_second(k, h, waits[h]) for h in range(2)]
        hook()
        for h in range(2):
            vector[h, points:ext] = borrow_end(k, h, waits[h])

    borrow(1, w0, lambda: reduce_next(0, 0))
    precondition(1, w0, m0)
    operate(1, m0, n0.at[:, own], [lambda: reduce_next(0, 1)])

    for h in range(2):
        alpha = reduced(0, h, 0) / reduced(0, h, 1)
        z1[h] = z0[h] - alpha * m0[h]
        w1[h, own] = w0[h, own] - alpha * n0[h, own]
        be[h, own] = be[h, own] - alpha * w0[h, own]
    reduce_open(1, lambda h: ((be[h, own], z1[h]), (z1[h], w1[h, own])))
    borrow(2, n0, lambda: reduce_next(1, 0))
    for h in range(2):
        alpha = reduced(0, h, 0) / reduced(0, h, 1)
        w1[h, points:ext] = w0[h, points:ext] - alpha * n0[h, points:ext]
    precondition(2, w1, m1)
    operate(2, m1, n1, [lambda: reduce_next(1, 1)])

    def steps(h):
        gamma0, delta0 = reduced(0, h, 0), reduced(0, h, 1)
        gamma1, delta1 = reduced(1, h, 0), reduced(1, h, 1)
        alpha0 = gamma0 / delta0
        beta1 = gamma1 / gamma0
        alpha1 = gamma1 / (delta1 - beta1 * gamma1 / alpha0)
        return alpha0, beta1, alpha1, gamma1

    result, got = ref["result"], ref["got"]

    for h in range(2):
        alpha0, beta1, alpha1, _ = steps(h)
        direction = z1[h] + beta1 * z0[h]
        image = w1[h, own] + beta1 * w0[h, own]
        result[0, h] = alpha0 * z0[h] + alpha1 * direction
        be[h, own] = be[h, own] - alpha1 * image
        z1[h] = z1[h] - alpha1 * (m1[h] + beta1 * m0[h])
        w1[h, own] = w1[h, own] - alpha1 * (n1[h] + beta1 * n0[h, own])
        z0[h] = direction
        w0[h, own] = image
    reduce_open(2, lambda h: ((be[h, own], z1[h]), (z1[h], w1[h, own])))
    for stage in range(len(groups)):
        reduce_next(2, stage)
    home = []
    for h in range(2):
        _, _, alpha1, gamma1 = steps(h)
        gamma2, delta2 = reduced(2, h, 0), reduced(2, h, 1)
        beta2 = gamma2 / gamma1
        alpha2 = gamma2 / (delta2 - beta2 * gamma2 / alpha1)
        result[0, h] = result[0, h] + alpha2 * (z1[h] + beta2 * z0[h])
        home.append(send(result.at[0, h], got.at[0, h], 0, 0, guard="traded", target=mate))
        result[1, h] = be[h, own] - alpha2 * (w1[h, own] + beta2 * w0[h, own])
        home.append(send(result.at[1, h], got.at[1, h], 0, 0, guard="traded", target=mate))

    @pl.when(kept)
    def _():
        for h in range(2):
            x_ref[:, half(h)] = result[0, h]
            r_ref[:, half(h)] = result[1, h]

    for n, wait in enumerate(home):
        wait()

        @pl.when(traded)
        def _():
            (x_ref, r_ref)[n % 2][:, half(n // 2)] = got[n % 2, n // 2]

    for which in (0, 1, -1, "traded"):
        def drain(descs=pending[which]):
            for desc in descs:
                desc.wait_send()
        guarded(which, drain)
    assert counter[0] <= cfg["copies"], counter[0]


def make(gx, gy, points, ov, rhs):
    ext = points + ov
    groups = ((1, 2, gy), (2, gx // 2, 1))
    each = [many * columns_too for _, many, columns_too in groups]
    copies = 8 + 7 + 3 * (16 + 8 + 8) + 3 * sum(n - 1 for n in each)
    stages = len(groups)
    half = (2, points, LANES)
    tall = (2, ext, LANES)
    shapes = {
        "send": pltpu.SemaphoreType.DMA((copies,)),
        "recv": pltpu.SemaphoreType.DMA((copies,)),
        "info_all": ((9, 8, points), F32),
        "gather": ((8 * ov, points), BF16),
        "scatter": ((points, 8 * ov), BF16),
        "ret": ((3, 2, 9, ov, LANES), F32),
        "ret_out": ((3, 2, ov, LANES), F32),
        "halo": ((3, 2, 2, points, LANES), F32),
        "part_out": ((3, 2, 3, points, LANES), F32),
        "part_in": ((3, 2, 2, points, LANES), F32),
        "give_out": ((3, 2, 9, ov, LANES), F32),
        "take_in": ((3, 2, 2, 3, ov, LANES), F32),
        "give_in": ((3, 2, 2, ov, LANES), F32),
        "pack": ((2, ext, 2 * LANES), BF16),
        "inverse": ((2, ext, ext), BF16),
        "blocks": ((2, 9, 2, points, points), BF16),
        "columns": ((3, points, 8), F32),
        "wide": ((8, ext), F32),
        "tall": ((ext, 8), F32),
        "matrix": ((ext, ext), F32),
        "full": ((ext, ext), F32),
        "leaf": ((256, 256), F32),
        "leaf_inverse": ((256, 256), F32),
        "reach": ((points, 256), F32),
        "result": ((2, 2, points, LANES), F32),
        "got": ((2, 2, points, LANES), F32),
        "sums": ((3, stages + 1, 8, LANES), F32),
        "gathered": ((3, sum(each), 8, LANES), F32),
        "be": (tall, F32), "w0": (tall, F32), "n0": (tall, F32), "w1": (tall, F32),
        "z0": (half, F32), "m0": (half, F32), "m1": (half, F32), "z1": (half, F32), "n1": (half, F32),
    }
    cfg = {"names": tuple(shapes), "points": points, "ov": ov, "gx": gx, "gy": gy, "groups": groups,
           "copies": copies, "leaves": (256,) * (points // 256) + (ov,)}
    scratch = [pltpu.VMEM(*v) if isinstance(v, tuple) else v for v in shapes.values()]
    whole = pl.BlockSpec(memory_space=pltpu.VMEM)
    call = pl.pallas_call(
        functools.partial(body, cfg),
        out_shape=(jax.ShapeDtypeStruct((points, rhs), F32),) * 2,
        in_specs=[whole, whole],
        out_specs=(whole, whole),
        scratch_shapes=scratch,
        compiler_params=pltpu.CompilerParams(
            collective_id=0, has_side_effects=True, vmem_limit_bytes=67043328),
    )

    def shards(right_side, coords, noise, intersect):
        ids = jnp.pad(intersect.reshape(1, ov).astype(F32), ((0, 0), (0, points - ov)))
        info = jnp.concatenate(
            [coords.reshape(2, points), noise.reshape(1, points), ids, jnp.zeros((4, points), F32)], axis=0)
        x, r = call(info, right_side.reshape(points, rhs))
        return x.reshape(right_side.shape), r.reshape(right_side.shape)

    return shards


def solution(mesh):
    gx, gy = mesh.shape["gx"], mesh.shape["gy"]

    def run(right_side, coords, noise, intersect):
        points, rhs = right_side.shape[2:]
        spec4, spec3 = P("gx", "gy", None, None), P("gx", "gy", None)
        return jax.shard_map(
            make(gx, gy, points, intersect.shape[2], rhs), mesh=mesh,
            in_specs=(spec4, spec4, spec3, spec3), out_specs=(spec4, spec4), check_vma=False,
        )(right_side, coords, noise, intersect)

    return run
```

```python
import functools
import math

import jax
import jax.numpy as jnp
from jax import lax
from jax.experimental import pallas as pl
from jax.experimental.pallas import tpu as pltpu
from jax.sharding import PartitionSpec as P

MESH = pl.DeviceIdType.MESH
HIGH = lax.Precision.HIGHEST
F32 = jnp.float32
BF16 = jnp.bfloat16
SCALE = math.sqrt(3.0) / 0.25
LEAST_NOISE = 0.25
NEWTON_STEPS = 7
LANES = 128
NEAR = [(a, b) for a in (-1, 0, 1) for b in (-1, 0, 1) if (a, b) != (0, 0)]
BOTH = (1, -1)


def slot(a, b):
    return (a + 1) * 3 + (b + 1)


def kernel_values(target_x, target_y, source_x, source_y):
    dx = target_x - source_x
    dy = target_y - source_y
    square = dx * dx + dy * dy
    distance = square * lax.rsqrt(jnp.maximum(square, 1e-30))
    scaled = SCALE * distance
    clipped = jnp.minimum(distance, 1.0)
    left = 1.0 - clipped
    square = left * left
    return (1.0 + scaled) * jnp.exp(-scaled) * (square * square * (4.0 * clipped + 1.0))


def halves(value):
    high = value.astype(BF16)
    low = (value - high.astype(F32)).astype(BF16)
    return high, low


def packed(value):
    return jnp.concatenate(halves(value), axis=1)


def bf_dot(left, right):
    return jnp.dot(left, right, preferred_element_type=F32)


def split_dot(high, low, both):
    first = bf_dot(high, both)
    return first[:, :LANES] + first[:, LANES:] + bf_dot(low, both[:, :LANES])


def pick_dot(chosen, both):
    first = bf_dot(chosen, both)
    return first[:, :LANES] + first[:, LANES:]


def three_dot(left, right):
    (left_high, left_low), (right_high, right_low) = halves(left), halves(right)
    return bf_dot(left_high, right_high) + bf_dot(left_high, right_low) + bf_dot(left_low, right_high)


def full_dot(left, right, dims=((1,), (0,))):
    return lax.dot_general(left, right, (dims, ((), ())), precision=HIGH, preferred_element_type=F32)


def identity(size):
    row = lax.broadcasted_iota(jnp.int32, (size, size), 0)
    return (row == lax.broadcasted_iota(jnp.int32, (size, size), 1)).astype(F32)


def newton_inverse(matrix, result):
    size = matrix.shape[0]
    value = matrix[...]
    largest = jnp.max(jnp.sum(jnp.abs(value), axis=1, keepdims=True), axis=0, keepdims=True)
    alpha = 1.0 / largest
    least = LEAST_NOISE * alpha
    scale = 2.0 / (1.0 + least)
    first = scale * alpha
    result[...] = (2.0 * first) * identity(size) - (first * first) * value

    def step(dot, least):
        scale = 2.0 / (1.0 + least)
        current = result[...]
        product = dot(matrix[...], current)
        result[...] = scale * dot(current, 2.0 * identity(size) - scale * product)
        return 4.0 * least / ((1.0 + least) * (1.0 + least))

    least = lax.fori_loop(0, NEWTON_STEPS - 1, lambda _, least: step(three_dot, least),
                          4.0 * least / ((1.0 + least) * (1.0 + least)))
    step(full_dot, least)


def body(cfg, coords_ref, noise_ref, ids_ref, b_ref, x_ref, r_ref, *scratch):
    ref = dict(zip(cfg["names"], scratch))
    points, ov = cfg["points"], cfg["ov"]
    ext = points + ov
    gx, gy = cfg["gx"], cfg["gy"]
    seat, col = lax.axis_index("gx"), lax.axis_index("gy")
    mid = gy // 2

    def trades(r, c):
        return (c // mid + r) % 2

    def host(r, c):
        return (r + trades(r, c) * (2 - 4 * ((r // 2) % 2)), c)

    row, _ = host(seat, col)
    traded, kept = trades(seat, col) == 1, trades(seat, col) == 0
    has = {0: None, 1: col < gy - 1, -1: col > 0, "traded": traded}
    send_sem, recv_sem = ref["send"], ref["recv"]
    counter = [0]
    pending = {0: [], 1: [], -1: [], "traded": []}
    latest = []

    def guarded(which, action):
        if which == 0:
            action()
        else:
            pl.when(has[which])(action)

    def device(a, b):
        return host((row + a + gx) % gx, (col + b + gy) % gy)

    def heir(a, b):
        return host((seat + a + gx) % gx, (col + b + gy) % gy)

    def holder(a, b):
        return ((row + a + gx) % gx, (col + b + gy) % gy)

    mate = (seat + 2 - 4 * ((seat // 2) % 2), col)

    def copy_to(src, dst, target):
        key = counter[0]
        counter[0] += 1
        return pltpu.make_async_remote_copy(
            src_ref=src, dst_ref=dst, send_sem=send_sem.at[key], recv_sem=recv_sem.at[key],
            device_id=target, device_id_type=MESH)

    def send(src, dst, a, b, guard=None, target=None):
        out = b if guard is None else guard
        arrives = -b if guard is None else guard
        desc = copy_to(src, dst, device(a, b) if target is None else target)
        guarded(out, desc.start)
        pending[out].append(desc)
        latest.append((out, desc))
        return functools.partial(guarded, arrives, desc.wait_recv)

    def sent(begin, end):
        for out, desc in latest[begin:end]:
            guarded(out, desc.wait_send)
            pending[out][:] = [other for other in pending[out] if other is not desc]

    info_ref = ref["info"]
    info_ref[...] = jnp.concatenate([
        coords_ref[...], noise_ref[...],
        jnp.concatenate([ids_ref[...].astype(F32), jnp.zeros((1, points - ov), F32)], axis=1),
        jnp.zeros((4, points), F32)], axis=0)

    info_all = ref["info_all"]
    for n in range(9):
        if n != 4:
            info_all[n] = jnp.full(info_all.shape[1:], -1.0, F32)

    @pl.when(kept)
    def _():
        info_all[4] = info_ref[...]

    @pl.when((col == 0) | (col == gy - 1))
    def _():
        for name in ("ret", "halo", "part_in", "take_in", "give_in"):
            buf = ref[name]
            flat = math.prod(buf.shape[:-2])
            for n in range(flat):
                index, rest = [], n
                for d in reversed(buf.shape[:-2]):
                    index.append(rest % d)
                    rest //= d
                buf[tuple(reversed(index))] = jnp.zeros(buf.shape[-2:], F32)

    groups = cfg["groups"]

    def partner(stride, many, columns_too, offset):
        position = (seat // stride) % many
        ahead = (position + offset % many) % many
        return (seat + (ahead - position) * stride, (col + offset // many) % gy if columns_too > 1 else col)

    barrier = pltpu.get_barrier_semaphore()
    for a, b in NEAR:
        for whom in (device, heir, holder):
            pl.semaphore_signal(barrier, inc=1, device_id=whom(a, b), device_id_type=MESH)
    pl.semaphore_signal(barrier, inc=1, device_id=mate, device_id_type=MESH)
    total = 3 * len(NEAR) + 1
    for group in groups:
        for offset in range(1, group[1] * group[2]):
            pl.semaphore_signal(barrier, inc=1, device_id=partner(*group, offset), device_id_type=MESH)
            total += 1
    pl.semaphore_wait(barrier, total)

    waits = [send(info_ref, info_all.at[slot(-a, -b)], a, b, target=heir(a, b)) for a, b in NEAR]
    waits.append(send(info_ref, info_all.at[4], 0, 0, guard="traded", target=mate))
    be = ref["be"]
    own = slice(0, points)

    def half(h):
        return slice(h * LANES, (h + 1) * LANES)

    came_right = [send(b_ref.at[:, half(h)], be.at[h, own], 0, 0, guard="traded", target=mate) for h in range(2)]

    @pl.when(kept)
    def _():
        for h in range(2):
            be[h, own] = b_ref[:, half(h)]

    for wait in waits:
        wait()

    gather, scatter = ref["gather"], ref["scatter"]

    def chosen_row(ids):
        sub = lax.broadcasted_iota(jnp.int32, (points, ov), 0).astype(F32)
        return (sub == ids).astype(F32).astype(BF16)

    def first_id(a, b):
        return float((3 * (1 - a) + (1 - b)) * points)

    def make_gather():
        for e, (a, b) in enumerate(NEAR):
            ids_col = jnp.transpose(info_all[slot(a, b), :, 0:ov])[:, 3:4] - first_id(a, b)
            lane = lax.broadcasted_iota(jnp.int32, (ov, points), 1).astype(F32)
            gather[e * ov:(e + 1) * ov, :] = (lane == ids_col).astype(F32).astype(BF16)

    def make_scatter():
        for e, (a, b) in enumerate(NEAR):
            scatter[:, e * ov:(e + 1) * ov] = chosen_row(info_all[slot(a, b), 3:4, 0:ov] - first_id(a, b))

    def borrow_first(k, h, own):
        out = ref["give_out"]
        asked = pick_dot(gather[...], packed(own))
        for e in range(8):
            a, b = NEAR[e]
            along, across = (a, b) if h == 0 else (b, a)
            out[k, h, slot(along, across)] = asked[e * ov:(e + 1) * ov]
        waits = []
        for step in BOTH:
            a, b = (step, 0) if h == 0 else (0, step)
            s = slot(step, -1)
            waits.append(send(out.at[k, h, s:s + 3], ref["take_in"].at[k, h, (1 - step) // 2], a, b))
        return waits

    def borrow_second(k, h, waits):
        for wait in waits:
            wait()
        out, came = ref["give_out"], ref["take_in"]
        waits = []
        for step in BOTH:
            mix = out.at[k, h, slot(0, step)]
            mix[...] = mix[...] + came[k, h, 0, step + 1] + came[k, h, 1, step + 1]
            a, b = (0, step) if h == 0 else (step, 0)
            waits.append(send(mix, ref["give_in"].at[k, h, (1 - step) // 2], a, b))
        return waits

    def borrow_end(k, h, waits):
        for wait in waits:
            wait()
        came, given = ref["take_in"], ref["give_in"]
        return came[k, h, 0, 1] + came[k, h, 1, 1] + given[k, h, 0] + given[k, h, 1]

    inverse = ref["inverse"]

    def precondition(k, extended, target, early=None, late=None):
        back, out = ref["ret"], ref["ret_out"]
        both, first = [], []
        for h in range(2):
            pack = ref["pack"].at[h]
            pack[...] = packed(extended[h])
            out[k, h] = split_dot(inverse[0, points:ext], inverse[1, points:ext], pack[...])
            waits = {}
            for a, b in ((0, 1), (0, -1), (1, 0), (-1, 0)):
                waits[a, b] = send(out.at[k, h], back.at[k, h, slot(-a, -b)], a, b)
            first.append(waits)

        def own_rows(h, carry):
            target[h] = split_dot(inverse[0, 0:points], inverse[1, 0:points], ref["pack"][h])
            return carry

        lax.fori_loop(0, 2, own_rows, 0)
        if early is not None:
            early()
        second = []
        for h in range(2):
            waits = []
            for step in BOTH:
                first[h][(0, step) if h == 0 else (step, 0)]()
            for step in BOTH:
                for other in BOTH:
                    if h == 0:
                        waits.append(send(back.at[k, h, slot(0, step)], back.at[k, h, slot(-other, step)],
                                          other, 0, guard=step))
                    else:
                        waits.append(send(back.at[k, h, slot(step, 0)], back.at[k, h, slot(step, -other)],
                                          0, other))
            for step in BOTH:
                waits.append(first[h][(step, 0) if h == 0 else (0, step)])
            second.append(waits)
        if late is not None:
            late()
        begin, leaving = len(latest), []
        for h in range(2):
            for wait in second[h]:
                wait()
            given = jnp.concatenate([packed(back[k, h, slot(a, b)]) for a, b in NEAR], axis=0)
            target[h] = target[h] + pick_dot(scatter[...], given)
            leaving.append([send(target.at[h], ref["halo"].at[k, h, (1 - step) // 2],
                                 *((step, 0) if h == 0 else (0, step))) for step in BOTH])
        return leaving, begin, len(latest)

    blocks = ref["blocks"]
    noise_col = ref["columns"]

    def operate(k, vector, target, started, hooks=(), early=None):
        halo, out, came = ref["halo"], ref["part_out"], ref["part_in"]
        waits, begin, end = started
        noise = noise_col[1, :, 2:3]
        for h in range(2):
            ref["pack"][h, own] = packed(vector[h])

        def from_here(n, carry):
            h, t = n // 3, n % 3
            out[k, h, t] = split_dot(blocks[h, 7 - 3 * t, 0], blocks[h, 7 - 3 * t, 1], ref["pack"][h, own])
            return carry

        lax.fori_loop(0, 6, from_here, 0)
        if early is not None:
            early()
        sources = ref["sources"]
        piece = points // 2

        def arrived(h, toward, rows):
            value = None
            for n, source in enumerate((-1, 1)):
                at = (toward + 1) * 3 + source + 1
                term = split_dot(blocks[h, at, 0, rows, :], blocks[h, at, 1, rows, :], sources[h, n])
                value = term if value is None else value + term
            return value

        def hand_on(h, rows):
            for toward in BOTH:
                part = out.at[k, h, 1 - toward, rows]
                part[...] = part[...] + arrived(h, toward, rows)
                a, b = (0, toward) if h == 0 else (toward, 0)
                later[h].append(send(part, came.at[k, h, (1 - toward) // 2, rows], a, b))

        later = [[], []]
        for h in range(2):
            for wait in waits[h]:
                wait()
            for n in range(2):
                sources[h, n] = packed(halo[k, h, n])
            hand_on(h, slice(0, piece))
        for h in range(2):
            hand_on(h, slice(piece, points))

        def own_sums(n, carry):
            h, rows = n // 2, pl.ds(pl.multiple_of(n % 2 * piece, piece), piece)
            out[k, h, 1, rows, :] = out[k, h, 1, rows, :] + arrived(h, 0, rows)
            return carry

        lax.fori_loop(0, 4, own_sums, 0)
        for hook in hooks:
            hook()
        for h in range(2):
            for wait in later[h]:
                wait()
            target[h] = (out[k, h, 1] + noise * vector[h]) + (came[k, h, 0] + came[k, h, 1])
        sent(begin, end)

    sums, gathered = ref["sums"], ref["gathered"]
    counts = [many * columns_too for _, many, columns_too in groups]
    offsets = [sum(counts[:g]) for g in range(len(groups))]
    open_waits = {}

    def reduce_start(k, stage):
        waits = []
        for offset in range(1, counts[stage]):
            desc = copy_to(sums.at[k, stage], gathered.at[k, offsets[stage] + offset],
                           partner(*groups[stage], offset))
            desc.start()
            pending[0].append(desc)
            waits.append(desc.wait_recv)
        open_waits[k] = waits

    def reduce_end(k, stage):
        for wait in open_waits[k]:
            wait()
        value = sums[k, stage]
        for offset in range(1, counts[stage]):
            value = value + gathered[k, offsets[stage] + offset]
        sums[k, stage + 1] = value

    def reduce_open(k, pairs):
        rows = []
        for h in range(2):
            for left, right in pairs(h):
                rows.append(jnp.sum(left * right, axis=0, keepdims=True))
        rows.append(jnp.zeros((4, LANES), F32))
        sums[k, 0] = jnp.concatenate(rows, axis=0)
        reduce_start(k, 0)

    def reduce_next(k, stage):
        reduce_end(k, stage)
        if stage + 1 < len(groups):
            reduce_start(k, stage + 1)

    def reduced(k, h, which):
        return sums[k, len(groups), 2 * h + which:2 * h + which + 1, :]

    w0, n0, w1 = ref["w0"], ref["n0"], ref["w1"]
    z0, m0, m1, z1, n1 = ref["z0"], ref["m0"], ref["m1"], ref["z1"], ref["n1"]
    columns = ref["columns"]
    for b in (-1, 0, 1):
        columns[b + 1] = jnp.transpose(info_all[slot(0, b)])
    ids = info_all[4, 3:4, 0:ov]
    picked = jnp.zeros((32, ov), F32)
    line = lax.broadcasted_iota(jnp.int32, (8, points), 0)
    for a, b in NEAR:
        shift = jnp.where(line == 0, float(a), jnp.where(line == 1, float(b), 0.0))
        value = info_all[slot(a, b)] + shift
        high, middle = halves(value)
        low = (value - high.astype(F32) - middle.astype(F32)).astype(BF16)
        pieces = jnp.concatenate([high.astype(F32), middle.astype(F32), low.astype(F32), jnp.zeros((8, points), F32)])
        picked = picked + bf_dot(pieces.astype(BF16), chosen_row(ids - float(slot(a, b) * points)))
    picked = (picked[0:8] + picked[8:16]) + picked[16:24]
    wide = ref["wide"]
    wide[:, own] = info_all[4]
    wide[:, points:ext] = picked
    tall = ref["tall"]
    tall[...] = jnp.transpose(wide[...])
    matrix = ref["matrix"]

    def ext_rows(c, carry):
        rows = pl.ds(pl.multiple_of(c * LANES, LANES), LANES)
        value = kernel_values(tall[rows, 0:1], tall[rows, 1:2], wide[0:1, :], wide[1:2, :])
        at = lax.broadcasted_iota(jnp.int32, (LANES, ext), 0) + c * LANES
        diag = at == lax.broadcasted_iota(jnp.int32, (LANES, ext), 1)
        matrix[rows, :] = value + jnp.where(diag, wide[2:3, :], 0.0)
        return carry

    lax.fori_loop(0, ext // LANES, ext_rows, 0)

    def build(count, pair):
        def block_rows(n, carry):
            b, a = pair(n // (points // LANES))
            rows = pl.ds(pl.multiple_of(n % (points // LANES) * LANES, LANES), LANES)
            source = info_all[3 * a + 4]
            value = kernel_values(columns[b + 1, rows, 0:1], columns[b + 1, rows, 1:2],
                                  source[0:1, :] + a.astype(F32), source[1:2, :] - b.astype(F32))
            high, low = halves(value)
            blocks[0, slot(b, a), 0, rows, :] = high
            blocks[0, slot(b, a), 1, rows, :] = low
            high, low = halves(jnp.transpose(value))
            blocks[1, slot(a, b), 0, :, rows] = high
            blocks[1, slot(a, b), 1, :, rows] = low
            return carry

        lax.fori_loop(0, count * (points // LANES), block_rows, 0)

    full = ref["full"]
    at = 0
    for size in cfg["leaves"]:
        now = slice(at, at + size)
        before = slice(0, at)
        leaf, leaf_inverse = ref["leaf"].at[0:size, 0:size], ref["leaf_inverse"].at[0:size, 0:size]
        if at == 0:
            leaf[...] = matrix[now, now]
            newton_inverse(leaf, leaf_inverse)
        else:
            cross = matrix[before, now]
            reach = ref["reach"].at[0:at, 0:size]
            reach[...] = full_dot(full[before, before], cross)
            leaf[...] = matrix[now, now] - full_dot(matrix[now, before], reach[...])
            newton_inverse(leaf, leaf_inverse)
            moved = full_dot(reach[...], leaf_inverse[...])
            full[before, before] = full[before, before] + full_dot(moved, reach[...], ((1,), (1,)))
            full[before, now] = -moved
            full[now, before] = -full_dot(leaf_inverse[...], reach[...], ((1,), (1,)))
        if at == 0:
            make_gather()
            for wait in came_right:
                wait()
            waits = [borrow_first(0, h, be[h, own]) for h in range(2)]
        elif at + size == points:
            waits = [borrow_second(0, h, waits[h]) for h in range(2)]
        full[now, now] = leaf_inverse[...]
        at += size
    high, low = halves(full[...])
    inverse[0] = high
    inverse[1] = low

    for h in range(2):
        be[h, points:ext] = borrow_end(0, h, waits[h])

    started = precondition(0, be, z0, early=lambda: build(3, lambda n: (n - 1, 0 * n)),
                           late=lambda: (make_scatter(), build(2, lambda n: (0 * n, 2 * n - 1))))
    operate(0, z0, w0.at[:, own], started,
            early=lambda: build(4, lambda n: (2 * (n // 2) - 1, 2 * (n % 2) - 1)))

    def borrow(k, vector, between):
        waits = [borrow_first(k, h, vector[h, own]) for h in range(2)]
        between()
        waits = [borrow_second(k, h, waits[h]) for h in range(2)]
        for h in range(2):
            vector[h, points:ext] = borrow_end(k, h, waits[h])

    borrow(1, w0, lambda: reduce_open(0, lambda h: ((be[h, own], z0[h]), (z0[h], w0[h, own]))))
    started = precondition(1, w0, m0)
    reduce_next(0, 0)
    operate(1, m0, n0.at[:, own], started, [lambda: reduce_next(0, 1)])

    def first_step():
        for h in range(2):
            alpha = reduced(0, h, 0) / reduced(0, h, 1)
            z1[h] = z0[h] - alpha * m0[h]
            w1[h, own] = w0[h, own] - alpha * n0[h, own]
            be[h, own] = be[h, own] - alpha * w0[h, own]
        reduce_open(1, lambda h: ((be[h, own], z1[h]), (z1[h], w1[h, own])))

    borrow(2, n0, first_step)
    for h in range(2):
        alpha = reduced(0, h, 0) / reduced(0, h, 1)
        w1[h, points:ext] = w0[h, points:ext] - alpha * n0[h, points:ext]
    started = precondition(2, w1, m1)
    reduce_next(1, 0)
    operate(2, m1, n1, started, [lambda: reduce_next(1, 1)])

    def steps(h):
        gamma0, delta0 = reduced(0, h, 0), reduced(0, h, 1)
        gamma1, delta1 = reduced(1, h, 0), reduced(1, h, 1)
        alpha0 = gamma0 / delta0
        beta1 = gamma1 / gamma0
        alpha1 = gamma1 / (delta1 - beta1 * gamma1 / alpha0)
        return alpha0, beta1, alpha1, gamma1

    result, got = ref["result"], ref["got"]

    for h in range(2):
        alpha0, beta1, alpha1, _ = steps(h)
        direction = z1[h] + beta1 * z0[h]
        image = w1[h, own] + beta1 * w0[h, own]
        result[0, h] = alpha0 * z0[h] + alpha1 * direction
        be[h, own] = be[h, own] - alpha1 * image
        z1[h] = z1[h] - alpha1 * (m1[h] + beta1 * m0[h])
        w1[h, own] = w1[h, own] - alpha1 * (n1[h] + beta1 * n0[h, own])
        z0[h] = direction
        w0[h, own] = image
    reduce_open(2, lambda h: ((be[h, own], z1[h]), (z1[h], w1[h, own])))
    for stage in range(len(groups)):
        reduce_next(2, stage)
    home = []
    for h in range(2):
        _, _, alpha1, gamma1 = steps(h)
        gamma2, delta2 = reduced(2, h, 0), reduced(2, h, 1)
        beta2 = gamma2 / gamma1
        alpha2 = gamma2 / (delta2 - beta2 * gamma2 / alpha1)
        result[0, h] = result[0, h] + alpha2 * (z1[h] + beta2 * z0[h])
        home.append(send(result.at[0, h], got.at[0, h], 0, 0, guard="traded", target=mate))
        result[1, h] = be[h, own] - alpha2 * (w1[h, own] + beta2 * w0[h, own])
        home.append(send(result.at[1, h], got.at[1, h], 0, 0, guard="traded", target=mate))

    @pl.when(kept)
    def _():
        for h in range(2):
            x_ref[:, half(h)] = result[0, h]
            r_ref[:, half(h)] = result[1, h]

    for n, wait in enumerate(home):
        wait()

        @pl.when(traded)
        def _():
            (x_ref, r_ref)[n % 2][:, half(n // 2)] = got[n % 2, n // 2]

    for which in (0, 1, -1, "traded"):
        def drain(descs=pending[which]):
            for desc in descs:
                desc.wait_send()
        guarded(which, drain)
    assert counter[0] <= cfg["copies"], counter[0]


def make(gx, gy, points, ov, rhs):
    ext = points + ov
    groups = ((1, 2, gy), (2, gx // 2, 1))
    each = [many * columns_too for _, many, columns_too in groups]
    copies = 8 + 7 + 3 * (16 + 12 + 8) + 3 * sum(n - 1 for n in each)
    stages = len(groups)
    half = (2, points, LANES)
    tall = (2, ext, LANES)
    shapes = {
        "send": pltpu.SemaphoreType.DMA((copies,)),
        "recv": pltpu.SemaphoreType.DMA((copies,)),
        "info": ((8, points), F32),
        "info_all": ((9, 8, points), F32),
        "gather": ((8 * ov, points), BF16),
        "scatter": ((points, 8 * ov), BF16),
        "ret": ((3, 2, 9, ov, LANES), F32),
        "ret_out": ((3, 2, ov, LANES), F32),
        "halo": ((3, 2, 2, points, LANES), F32),
        "part_out": ((3, 2, 3, points, LANES), F32),
        "part_in": ((3, 2, 2, points, LANES), F32),
        "give_out": ((3, 2, 9, ov, LANES), F32),
        "take_in": ((3, 2, 2, 3, ov, LANES), F32),
        "give_in": ((3, 2, 2, ov, LANES), F32),
        "pack": ((2, ext, 2 * LANES), BF16),
        "inverse": ((2, ext, ext), BF16),
        "blocks": ((2, 9, 2, points, points), BF16),
        "sources": ((2, 2, points, 2 * LANES), BF16),
        "columns": ((3, points, 8), F32),
        "wide": ((8, ext), F32),
        "tall": ((ext, 8), F32),
        "matrix": ((ext, ext), F32),
        "full": ((ext, ext), F32),
        "leaf": ((256, 256), F32),
        "leaf_inverse": ((256, 256), F32),
        "reach": ((points, 256), F32),
        "result": ((2, 2, points, LANES), F32),
        "got": ((2, 2, points, LANES), F32),
        "sums": ((3, stages + 1, 8, LANES), F32),
        "gathered": ((3, sum(each), 8, LANES), F32),
        "be": (tall, F32), "w0": (tall, F32), "n0": (tall, F32), "w1": (tall, F32),
        "z0": (half, F32), "m0": (half, F32), "m1": (half, F32), "z1": (half, F32), "n1": (half, F32),
    }
    cfg = {"names": tuple(shapes), "points": points, "ov": ov, "gx": gx, "gy": gy, "groups": groups,
           "copies": copies, "leaves": (256,) * (points // 256) + (ov,)}
    scratch = [pltpu.VMEM(*v) if isinstance(v, tuple) else v for v in shapes.values()]
    whole = pl.BlockSpec(memory_space=pltpu.VMEM)
    call = pl.pallas_call(
        functools.partial(body, cfg),
        out_shape=(jax.ShapeDtypeStruct((points, rhs), F32),) * 2,
        in_specs=[whole] * 4,
        out_specs=(whole, whole),
        scratch_shapes=scratch,
        compiler_params=pltpu.CompilerParams(
            collective_id=0, has_side_effects=True, vmem_limit_bytes=67043328),
    )

    def shards(right_side, coords, noise, intersect):
        x, r = call(coords.reshape(2, points), noise.reshape(1, points), intersect.reshape(1, ov),
                    right_side.reshape(points, rhs))
        return x.reshape(right_side.shape), r.reshape(right_side.shape)

    return shards


def solution(mesh):
    gx, gy = mesh.shape["gx"], mesh.shape["gy"]

    def run(right_side, coords, noise, intersect):
        points, rhs = right_side.shape[2:]
        spec4, spec3 = P("gx", "gy", None, None), P("gx", "gy", None)
        return jax.shard_map(
            make(gx, gy, points, intersect.shape[2], rhs), mesh=mesh,
            in_specs=(spec4, spec4, spec3, spec3), out_specs=(spec4, spec4), check_vma=False,
        )(right_side, coords, noise, intersect)

    return run
```

```python
import functools
import math

import jax
import jax.numpy as jnp
from jax import lax
from jax.experimental import pallas as pl
from jax.experimental.pallas import tpu as pltpu
from jax.sharding import PartitionSpec as P

MESH = pl.DeviceIdType.MESH
HIGH = lax.Precision.HIGHEST
F32 = jnp.float32
BF16 = jnp.bfloat16
SCALE = math.sqrt(3.0) / 0.25
LEAST_NOISE = 0.25
NEWTON_STEPS = 7
LANES = 128
NEAR = [(a, b) for a in (-1, 0, 1) for b in (-1, 0, 1) if (a, b) != (0, 0)]
BOTH = (1, -1)


def slot(a, b):
    return (a + 1) * 3 + (b + 1)


def kernel_values(target_x, target_y, source_x, source_y):
    dx = target_x - source_x
    dy = target_y - source_y
    square = dx * dx + dy * dy
    distance = square * lax.rsqrt(jnp.maximum(square, 1e-30))
    scaled = SCALE * distance
    clipped = jnp.minimum(distance, 1.0)
    left = 1.0 - clipped
    square = left * left
    return (1.0 + scaled) * jnp.exp(-scaled) * (square * square * (4.0 * clipped + 1.0))


def halves(value):
    high = value.astype(BF16)
    low = (value - high.astype(F32)).astype(BF16)
    return high, low


def packed(value):
    return jnp.concatenate(halves(value), axis=1)


def bf_dot(left, right):
    return jnp.dot(left, right, preferred_element_type=F32)


def split_dot(high, low, both):
    first = bf_dot(high, both)
    return first[:, :LANES] + first[:, LANES:] + bf_dot(low, both[:, :LANES])


def pick_dot(chosen, both):
    first = bf_dot(chosen, both)
    return first[:, :LANES] + first[:, LANES:]


def three_dot(left, right):
    (left_high, left_low), (right_high, right_low) = halves(left), halves(right)
    return bf_dot(left_high, right_high) + bf_dot(left_high, right_low) + bf_dot(left_low, right_high)


def full_dot(left, right, dims=((1,), (0,))):
    return lax.dot_general(left, right, (dims, ((), ())), precision=HIGH, preferred_element_type=F32)


def identity(size):
    row = lax.broadcasted_iota(jnp.int32, (size, size), 0)
    return (row == lax.broadcasted_iota(jnp.int32, (size, size), 1)).astype(F32)


def newton_inverse(matrix, result):
    size = matrix.shape[0]
    value = matrix[...]
    largest = jnp.max(jnp.sum(jnp.abs(value), axis=1, keepdims=True), axis=0, keepdims=True)
    alpha = 1.0 / largest
    least = LEAST_NOISE * alpha
    scale = 2.0 / (1.0 + least)
    first = scale * alpha
    result[...] = (2.0 * first) * identity(size) - (first * first) * value

    def step(dot, least):
        scale = 2.0 / (1.0 + least)
        current = result[...]
        product = dot(matrix[...], current)
        result[...] = scale * dot(current, 2.0 * identity(size) - scale * product)
        return 4.0 * least / ((1.0 + least) * (1.0 + least))

    least = lax.fori_loop(0, NEWTON_STEPS - 1, lambda _, least: step(three_dot, least),
                          4.0 * least / ((1.0 + least) * (1.0 + least)))
    step(full_dot, least)


def body(cfg, coords_ref, noise_ref, ids_ref, b_ref, x_ref, r_ref, *scratch):
    ref = dict(zip(cfg["names"], scratch))
    points, ov = cfg["points"], cfg["ov"]
    ext = points + ov
    gx, gy = cfg["gx"], cfg["gy"]
    seat, col = lax.axis_index("gx"), lax.axis_index("gy")
    mid = gy // 2

    def trades(r, c):
        return (c // mid + r) % 2

    def host(r, c):
        return (r + trades(r, c) * (2 - 4 * ((r // 2) % 2)), c)

    row, _ = host(seat, col)
    traded, kept = trades(seat, col) == 1, trades(seat, col) == 0
    has = {0: None, 1: col < gy - 1, -1: col > 0, "traded": traded}
    send_sem, recv_sem = ref["send"], ref["recv"]
    counter = [0]
    pending = {0: [], 1: [], -1: [], "traded": []}
    latest = []

    def guarded(which, action):
        if which == 0:
            action()
        else:
            pl.when(has[which])(action)

    def device(a, b):
        return host((row + a + gx) % gx, (col + b + gy) % gy)

    def heir(a, b):
        return host((seat + a + gx) % gx, (col + b + gy) % gy)

    def holder(a, b):
        return ((row + a + gx) % gx, (col + b + gy) % gy)

    mate = (seat + 2 - 4 * ((seat // 2) % 2), col)

    def copy_to(src, dst, target):
        key = counter[0]
        counter[0] += 1
        return pltpu.make_async_remote_copy(
            src_ref=src, dst_ref=dst, send_sem=send_sem.at[key], recv_sem=recv_sem.at[key],
            device_id=target, device_id_type=MESH)

    def send(src, dst, a, b, guard=None, target=None):
        out = b if guard is None else guard
        arrives = -b if guard is None else guard
        desc = copy_to(src, dst, device(a, b) if target is None else target)
        guarded(out, desc.start)
        pending[out].append(desc)
        latest.append((out, desc))
        return functools.partial(guarded, arrives, desc.wait_recv)

    def sent(begin, end):
        for out, desc in latest[begin:end]:
            guarded(out, desc.wait_send)
            pending[out][:] = [other for other in pending[out] if other is not desc]

    info_ref = ref["info"]
    info_ref[...] = jnp.concatenate([
        coords_ref[...], noise_ref[...],
        jnp.concatenate([ids_ref[...].astype(F32), jnp.zeros((1, points - ov), F32)], axis=1),
        jnp.zeros((4, points), F32)], axis=0)

    info_all = ref["info_all"]
    for n in range(9):
        if n != 4:
            info_all[n] = jnp.full(info_all.shape[1:], -1.0, F32)

    @pl.when(kept)
    def _():
        info_all[4] = info_ref[...]

    @pl.when((col == 0) | (col == gy - 1))
    def _():
        for name in ("ret", "halo", "part_in", "take_in", "give_in"):
            buf = ref[name]
            flat = math.prod(buf.shape[:-2])
            for n in range(flat):
                index, rest = [], n
                for d in reversed(buf.shape[:-2]):
                    index.append(rest % d)
                    rest //= d
                buf[tuple(reversed(index))] = jnp.zeros(buf.shape[-2:], F32)

    groups = cfg["groups"]

    def partner(group, offset):
        line, pair, core = seat // 4, (seat // 2) % 2, seat % 2
        if group == "plane":
            pair, other = (pair + offset % 2) % 2, (col + offset // 2) % gy
            return (4 * line + 2 * pair + core, other)
        core, line = (core + offset % 2) % 2, (line + offset // 2) % (gx // 4)
        return (4 * line + 2 * pair + core, col)

    barrier = pltpu.get_barrier_semaphore()
    for a, b in NEAR:
        for whom in (device, heir, holder):
            pl.semaphore_signal(barrier, inc=1, device_id=whom(a, b), device_id_type=MESH)
    pl.semaphore_signal(barrier, inc=1, device_id=mate, device_id_type=MESH)
    total = 3 * len(NEAR) + 1
    for group in groups:
        for offset in range(1, group[1]):
            pl.semaphore_signal(barrier, inc=1, device_id=partner(group[0], offset), device_id_type=MESH)
            total += 1
    pl.semaphore_wait(barrier, total)

    waits = [send(info_ref, info_all.at[slot(-a, -b)], a, b, target=heir(a, b)) for a, b in NEAR]
    waits.append(send(info_ref, info_all.at[4], 0, 0, guard="traded", target=mate))
    be = ref["be"]
    own = slice(0, points)

    def half(h):
        return slice(h * LANES, (h + 1) * LANES)

    came_right = [send(b_ref.at[:, half(h)], be.at[h, own], 0, 0, guard="traded", target=mate) for h in range(2)]

    @pl.when(kept)
    def _():
        for h in range(2):
            be[h, own] = b_ref[:, half(h)]

    for wait in waits:
        wait()

    gather, scatter = ref["gather"], ref["scatter"]

    def chosen_row(ids):
        sub = lax.broadcasted_iota(jnp.int32, (points, ov), 0).astype(F32)
        return (sub == ids).astype(F32).astype(BF16)

    def first_id(a, b):
        return float((3 * (1 - a) + (1 - b)) * points)

    def make_gather():
        for e, (a, b) in enumerate(NEAR):
            ids_col = jnp.transpose(info_all[slot(a, b), :, 0:ov])[:, 3:4] - first_id(a, b)
            lane = lax.broadcasted_iota(jnp.int32, (ov, points), 1).astype(F32)
            gather[e * ov:(e + 1) * ov, :] = (lane == ids_col).astype(F32).astype(BF16)

    def make_scatter():
        for e, (a, b) in enumerate(NEAR):
            scatter[:, e * ov:(e + 1) * ov] = chosen_row(info_all[slot(a, b), 3:4, 0:ov] - first_id(a, b))

    def borrow_first(k, h, own):
        out = ref["give_out"]
        asked = pick_dot(gather[...], packed(own))
        for e in range(8):
            a, b = NEAR[e]
            along, across = (a, b) if h == 0 else (b, a)
            out[k, h, slot(along, across)] = asked[e * ov:(e + 1) * ov]
        waits = []
        for step in BOTH:
            a, b = (step, 0) if h == 0 else (0, step)
            s = slot(step, -1)
            waits.append(send(out.at[k, h, s:s + 3], ref["take_in"].at[k, h, (1 - step) // 2], a, b))
        return waits

    def borrow_second(k, h, waits):
        for wait in waits:
            wait()
        out, came = ref["give_out"], ref["take_in"]
        waits = []
        for step in BOTH:
            mix = out.at[k, h, slot(0, step)]
            mix[...] = mix[...] + came[k, h, 0, step + 1] + came[k, h, 1, step + 1]
            a, b = (0, step) if h == 0 else (step, 0)
            waits.append(send(mix, ref["give_in"].at[k, h, (1 - step) // 2], a, b))
        return waits

    def borrow_end(k, h, waits):
        for wait in waits:
            wait()
        came, given = ref["take_in"], ref["give_in"]
        return came[k, h, 0, 1] + came[k, h, 1, 1] + given[k, h, 0] + given[k, h, 1]

    inverse = ref["inverse"]

    def precondition(k, extended, target, early=None, late=None):
        back, out = ref["ret"], ref["ret_out"]
        both, first = [], []
        for h in range(2):
            pack = ref["pack"].at[h]
            pack[...] = packed(extended[h])
            out[k, h] = split_dot(inverse[0, points:ext], inverse[1, points:ext], pack[...])
            waits = {}
            for a, b in ((0, 1), (0, -1), (1, 0), (-1, 0)):
                waits[a, b] = send(out.at[k, h], back.at[k, h, slot(-a, -b)], a, b)
            first.append(waits)

        def own_rows(h, carry):
            target[h] = split_dot(inverse[0, 0:points], inverse[1, 0:points], ref["pack"][h])
            return carry

        lax.fori_loop(0, 2, own_rows, 0)
        if early is not None:
            early()
        second = []
        for h in range(2):
            waits = []
            for step in BOTH:
                first[h][(0, step) if h == 0 else (step, 0)]()
            for step in BOTH:
                for other in BOTH:
                    if h == 0:
                        waits.append(send(back.at[k, h, slot(0, step)], back.at[k, h, slot(-other, step)],
                                          other, 0, guard=step))
                    else:
                        waits.append(send(back.at[k, h, slot(step, 0)], back.at[k, h, slot(step, -other)],
                                          0, other))
            for step in BOTH:
                waits.append(first[h][(step, 0) if h == 0 else (0, step)])
            second.append(waits)
        if late is not None:
            late()
        begin, leaving = len(latest), []
        for h in range(2):
            for wait in second[h]:
                wait()
            given = jnp.concatenate([packed(back[k, h, slot(a, b)]) for a, b in NEAR], axis=0)
            target[h] = target[h] + pick_dot(scatter[...], given)
            leaving.append([send(target.at[h], ref["halo"].at[k, h, (1 - step) // 2],
                                 *((step, 0) if h == 0 else (0, step))) for step in BOTH])
        return leaving, begin, len(latest)

    blocks = ref["blocks"]
    noise_col = ref["columns"]

    def operate(k, vector, target, started, hooks=(), early=None):
        halo, out, came = ref["halo"], ref["part_out"], ref["part_in"]
        waits, begin, end = started
        noise = noise_col[1, :, 2:3]
        for h in range(2):
            ref["pack"][h, own] = packed(vector[h])

        def from_here(n, carry):
            h, t = n // 3, n % 3
            out[k, h, t] = split_dot(blocks[h, 7 - 3 * t, 0], blocks[h, 7 - 3 * t, 1], ref["pack"][h, own])
            return carry

        lax.fori_loop(0, 6, from_here, 0)
        if early is not None:
            early()
        sources = ref["sources"]
        piece = points // 2

        def arrived(h, toward, rows):
            value = None
            for n, source in enumerate((-1, 1)):
                at = (toward + 1) * 3 + source + 1
                term = split_dot(blocks[h, at, 0, rows, :], blocks[h, at, 1, rows, :], sources[h, n])
                value = term if value is None else value + term
            return value

        def hand_on(h, rows):
            for toward in BOTH:
                part = out.at[k, h, 1 - toward, rows]
                part[...] = part[...] + arrived(h, toward, rows)
                a, b = (0, toward) if h == 0 else (toward, 0)
                later[h].append(send(part, came.at[k, h, (1 - toward) // 2, rows], a, b))

        later = [[], []]
        for h in range(2):
            for wait in waits[h]:
                wait()
            for n in range(2):
                sources[h, n] = packed(halo[k, h, n])
            hand_on(h, slice(0, piece))
        for h in range(2):
            hand_on(h, slice(piece, points))

        def own_sums(n, carry):
            h, rows = n // 2, pl.ds(pl.multiple_of(n % 2 * piece, piece), piece)
            out[k, h, 1, rows, :] = out[k, h, 1, rows, :] + arrived(h, 0, rows)
            return carry

        lax.fori_loop(0, 4, own_sums, 0)
        for hook in hooks:
            hook()
        for h in range(2):
            for wait in later[h]:
                wait()
            target[h] = (out[k, h, 1] + noise * vector[h]) + (came[k, h, 0] + came[k, h, 1])
        sent(begin, end)

    sums, gathered = ref["sums"], ref["gathered"]
    counts = [count for _, count in groups]
    offsets = [sum(counts[:g]) for g in range(len(groups))]
    open_waits = {}

    def reduce_start(k, stage):
        waits = []
        for offset in range(1, counts[stage]):
            desc = copy_to(sums.at[k, stage], gathered.at[k, offsets[stage] + offset],
                           partner(groups[stage][0], offset))
            desc.start()
            pending[0].append(desc)
            waits.append(desc.wait_recv)
        open_waits[k] = waits

    def reduce_end(k, stage):
        for wait in open_waits[k]:
            wait()
        value = sums[k, stage]
        for offset in range(1, counts[stage]):
            value = value + gathered[k, offsets[stage] + offset]
        sums[k, stage + 1] = value

    def reduce_open(k, pairs):
        rows = []
        for h in range(2):
            for left, right in pairs(h):
                rows.append(jnp.sum(left * right, axis=0, keepdims=True))
        rows.append(jnp.zeros((4, LANES), F32))
        sums[k, 0] = jnp.concatenate(rows, axis=0)
        reduce_start(k, 0)

    def reduce_next(k, stage):
        reduce_end(k, stage)
        if stage + 1 < len(groups):
            reduce_start(k, stage + 1)

    def reduced(k, h, which):
        return sums[k, len(groups), 2 * h + which:2 * h + which + 1, :]

    w0, n0, w1 = ref["w0"], ref["n0"], ref["w1"]
    z0, m0, m1, z1, n1 = ref["z0"], ref["m0"], ref["m1"], ref["z1"], ref["n1"]
    columns = ref["columns"]
    for b in (-1, 0, 1):
        columns[b + 1] = jnp.transpose(info_all[slot(0, b)])
    ids = info_all[4, 3:4, 0:ov]
    picked = jnp.zeros((32, ov), F32)
    line = lax.broadcasted_iota(jnp.int32, (8, points), 0)
    for a, b in NEAR:
        shift = jnp.where(line == 0, float(a), jnp.where(line == 1, float(b), 0.0))
        value = info_all[slot(a, b)] + shift
        high, middle = halves(value)
        low = (value - high.astype(F32) - middle.astype(F32)).astype(BF16)
        pieces = jnp.concatenate([high.astype(F32), middle.astype(F32), low.astype(F32), jnp.zeros((8, points), F32)])
        picked = picked + bf_dot(pieces.astype(BF16), chosen_row(ids - float(slot(a, b) * points)))
    picked = (picked[0:8] + picked[8:16]) + picked[16:24]
    wide = ref["wide"]
    wide[:, own] = info_all[4]
    wide[:, points:ext] = picked
    tall = ref["tall"]
    tall[...] = jnp.transpose(wide[...])
    matrix = ref["matrix"]

    def ext_rows(c, carry):
        rows = pl.ds(pl.multiple_of(c * LANES, LANES), LANES)
        value = kernel_values(tall[rows, 0:1], tall[rows, 1:2], wide[0:1, :], wide[1:2, :])
        at = lax.broadcasted_iota(jnp.int32, (LANES, ext), 0) + c * LANES
        diag = at == lax.broadcasted_iota(jnp.int32, (LANES, ext), 1)
        matrix[rows, :] = value + jnp.where(diag, wide[2:3, :], 0.0)
        return carry

    lax.fori_loop(0, ext // LANES, ext_rows, 0)

    def build(count, pair):
        def block_rows(n, carry):
            b, a = pair(n // (points // LANES))
            rows = pl.ds(pl.multiple_of(n % (points // LANES) * LANES, LANES), LANES)
            source = info_all[3 * a + 4]
            value = kernel_values(columns[b + 1, rows, 0:1], columns[b + 1, rows, 1:2],
                                  source[0:1, :] + a.astype(F32), source[1:2, :] - b.astype(F32))
            high, low = halves(value)
            blocks[0, slot(b, a), 0, rows, :] = high
            blocks[0, slot(b, a), 1, rows, :] = low
            high, low = halves(jnp.transpose(value))
            blocks[1, slot(a, b), 0, :, rows] = high
            blocks[1, slot(a, b), 1, :, rows] = low
            return carry

        lax.fori_loop(0, count * (points // LANES), block_rows, 0)

    full = ref["full"]
    at = 0
    for size in cfg["leaves"]:
        now = slice(at, at + size)
        before = slice(0, at)
        leaf, leaf_inverse = ref["leaf"].at[0:size, 0:size], ref["leaf_inverse"].at[0:size, 0:size]
        if at == 0:
            leaf[...] = matrix[now, now]
            newton_inverse(leaf, leaf_inverse)
        else:
            cross = matrix[before, now]
            reach = ref["reach"].at[0:at, 0:size]
            reach[...] = full_dot(full[before, before], cross)
            leaf[...] = matrix[now, now] - full_dot(matrix[now, before], reach[...])
            newton_inverse(leaf, leaf_inverse)
            moved = full_dot(reach[...], leaf_inverse[...])
            full[before, before] = full[before, before] + full_dot(moved, reach[...], ((1,), (1,)))
            full[before, now] = -moved
            full[now, before] = -full_dot(leaf_inverse[...], reach[...], ((1,), (1,)))
        if at == 0:
            make_gather()
            for wait in came_right:
                wait()
            waits = [borrow_first(0, h, be[h, own]) for h in range(2)]
        elif at + size == points:
            waits = [borrow_second(0, h, waits[h]) for h in range(2)]
        full[now, now] = leaf_inverse[...]
        at += size
    high, low = halves(full[...])
    inverse[0] = high
    inverse[1] = low

    for h in range(2):
        be[h, points:ext] = borrow_end(0, h, waits[h])

    started = precondition(0, be, z0, early=lambda: build(3, lambda n: (n - 1, 0 * n)),
                           late=lambda: (make_scatter(), build(2, lambda n: (0 * n, 2 * n - 1))))
    operate(0, z0, w0.at[:, own], started,
            early=lambda: build(4, lambda n: (2 * (n // 2) - 1, 2 * (n % 2) - 1)))

    def borrow(k, vector, between):
        waits = [borrow_first(k, h, vector[h, own]) for h in range(2)]
        between()
        waits = [borrow_second(k, h, waits[h]) for h in range(2)]
        for h in range(2):
            vector[h, points:ext] = borrow_end(k, h, waits[h])

    borrow(1, w0, lambda: reduce_open(0, lambda h: ((be[h, own], z0[h]), (z0[h], w0[h, own]))))
    started = precondition(1, w0, m0)
    reduce_next(0, 0)
    operate(1, m0, n0.at[:, own], started, [lambda: reduce_next(0, 1)])

    def first_step():
        for h in range(2):
            alpha = reduced(0, h, 0) / reduced(0, h, 1)
            z1[h] = z0[h] - alpha * m0[h]
            w1[h, own] = w0[h, own] - alpha * n0[h, own]
            be[h, own] = be[h, own] - alpha * w0[h, own]
        reduce_open(1, lambda h: ((be[h, own], z1[h]), (z1[h], w1[h, own])))

    borrow(2, n0, first_step)
    for h in range(2):
        alpha = reduced(0, h, 0) / reduced(0, h, 1)
        w1[h, points:ext] = w0[h, points:ext] - alpha * n0[h, points:ext]
    started = precondition(2, w1, m1)
    reduce_next(1, 0)

    def steps(h):
        gamma0, delta0 = reduced(0, h, 0), reduced(0, h, 1)
        gamma1, delta1 = reduced(1, h, 0), reduced(1, h, 1)
        alpha0 = gamma0 / delta0
        beta1 = gamma1 / gamma0
        alpha1 = gamma1 / (delta1 - beta1 * gamma1 / alpha0)
        return alpha0, beta1, alpha1, gamma1

    result, got = ref["result"], ref["got"]

    def second_step():
        for h in range(2):
            alpha0, beta1, alpha1, _ = steps(h)
            direction = z1[h] + beta1 * z0[h]
            image = w1[h, own] + beta1 * w0[h, own]
            result[0, h] = alpha0 * z0[h] + alpha1 * direction
            be[h, own] = be[h, own] - alpha1 * image
            z1[h] = z1[h] - alpha1 * (m1[h] + beta1 * m0[h])
            w1[h, own] = w1[h, own] - (alpha1 * beta1) * n0[h, own]
            z0[h] = direction
            w0[h, own] = image

    operate(2, m1, n1, started, [lambda: reduce_next(1, 1), second_step])
    for h in range(2):
        w1[h, own] = w1[h, own] - steps(h)[2] * n1[h]
    reduce_open(2, lambda h: ((be[h, own], z1[h]), (z1[h], w1[h, own])))
    for stage in range(len(groups)):
        reduce_next(2, stage)
    home = []
    for h in range(2):
        _, _, alpha1, gamma1 = steps(h)
        gamma2, delta2 = reduced(2, h, 0), reduced(2, h, 1)
        beta2 = gamma2 / gamma1
        alpha2 = gamma2 / (delta2 - beta2 * gamma2 / alpha1)
        result[0, h] = result[0, h] + alpha2 * (z1[h] + beta2 * z0[h])
        home.append(send(result.at[0, h], got.at[0, h], 0, 0, guard="traded", target=mate))
        result[1, h] = be[h, own] - alpha2 * (w1[h, own] + beta2 * w0[h, own])
        home.append(send(result.at[1, h], got.at[1, h], 0, 0, guard="traded", target=mate))

    @pl.when(kept)
    def _():
        for h in range(2):
            x_ref[:, half(h)] = result[0, h]
            r_ref[:, half(h)] = result[1, h]

    for n, wait in enumerate(home):
        wait()

        @pl.when(traded)
        def _():
            (x_ref, r_ref)[n % 2][:, half(n // 2)] = got[n % 2, n // 2]

    for which in (0, 1, -1, "traded"):
        def drain(descs=pending[which]):
            for desc in descs:
                desc.wait_send()
        guarded(which, drain)
    assert counter[0] <= cfg["copies"], counter[0]


def make(gx, gy, points, ov, rhs):
    ext = points + ov
    groups = (("plane", 2 * gy), ("line", gx // 2))
    each = [count for _, count in groups]
    copies = 8 + 7 + 3 * (16 + 12 + 8) + 3 * sum(n - 1 for n in each)
    stages = len(groups)
    half = (2, points, LANES)
    tall = (2, ext, LANES)
    shapes = {
        "send": pltpu.SemaphoreType.DMA((copies,)),
        "recv": pltpu.SemaphoreType.DMA((copies,)),
        "info": ((8, points), F32),
        "info_all": ((9, 8, points), F32),
        "gather": ((8 * ov, points), BF16),
        "scatter": ((points, 8 * ov), BF16),
        "ret": ((3, 2, 9, ov, LANES), F32),
        "ret_out": ((3, 2, ov, LANES), F32),
        "halo": ((3, 2, 2, points, LANES), F32),
        "part_out": ((3, 2, 3, points, LANES), F32),
        "part_in": ((3, 2, 2, points, LANES), F32),
        "give_out": ((3, 2, 9, ov, LANES), F32),
        "take_in": ((3, 2, 2, 3, ov, LANES), F32),
        "give_in": ((3, 2, 2, ov, LANES), F32),
        "pack": ((2, ext, 2 * LANES), BF16),
        "inverse": ((2, ext, ext), BF16),
        "blocks": ((2, 9, 2, points, points), BF16),
        "sources": ((2, 2, points, 2 * LANES), BF16),
        "columns": ((3, points, 8), F32),
        "wide": ((8, ext), F32),
        "tall": ((ext, 8), F32),
        "matrix": ((ext, ext), F32),
        "full": ((ext, ext), F32),
        "leaf": ((256, 256), F32),
        "leaf_inverse": ((256, 256), F32),
        "reach": ((points, 256), F32),
        "result": ((2, 2, points, LANES), F32),
        "got": ((2, 2, points, LANES), F32),
        "sums": ((3, stages + 1, 8, LANES), F32),
        "gathered": ((3, sum(each), 8, LANES), F32),
        "be": (tall, F32), "w0": (tall, F32), "n0": (tall, F32), "w1": (tall, F32),
        "z0": (half, F32), "m0": (half, F32), "m1": (half, F32), "z1": (half, F32), "n1": (half, F32),
    }
    cfg = {"names": tuple(shapes), "points": points, "ov": ov, "gx": gx, "gy": gy, "groups": groups,
           "copies": copies, "leaves": (256,) * (points // 256) + (ov,)}
    scratch = [pltpu.VMEM(*v) if isinstance(v, tuple) else v for v in shapes.values()]
    whole = pl.BlockSpec(memory_space=pltpu.VMEM)
    call = pl.pallas_call(
        functools.partial(body, cfg),
        out_shape=(jax.ShapeDtypeStruct((points, rhs), F32),) * 2,
        in_specs=[whole] * 4,
        out_specs=(whole, whole),
        scratch_shapes=scratch,
        compiler_params=pltpu.CompilerParams(
            collective_id=0, has_side_effects=True, vmem_limit_bytes=67043328),
    )

    def shards(right_side, coords, noise, intersect):
        x, r = call(coords.reshape(2, points), noise.reshape(1, points), intersect.reshape(1, ov),
                    right_side.reshape(points, rhs))
        return x.reshape(right_side.shape), r.reshape(right_side.shape)

    return shards


def solution(mesh):
    gx, gy = mesh.shape["gx"], mesh.shape["gy"]

    def run(right_side, coords, noise, intersect):
        points, rhs = right_side.shape[2:]
        spec4, spec3 = P("gx", "gy", None, None), P("gx", "gy", None)
        return jax.shard_map(
            make(gx, gy, points, intersect.shape[2], rhs), mesh=mesh,
            in_specs=(spec4, spec4, spec3, spec3), out_specs=(spec4, spec4), check_vma=False,
        )(right_side, coords, noise, intersect)

    return run
```

```python
import functools
import math

import jax
import jax.numpy as jnp
from jax import lax
from jax.experimental import pallas as pl
from jax.experimental.pallas import tpu as pltpu
from jax.sharding import PartitionSpec as P

MESH = pl.DeviceIdType.MESH
HIGH = lax.Precision.HIGHEST
F32 = jnp.float32
BF16 = jnp.bfloat16
SCALE = math.sqrt(3.0) / 0.25
LEAST_NOISE = 0.25
NEWTON_STEPS = 7
LANES = 128
NEAR = [(a, b) for a in (-1, 0, 1) for b in (-1, 0, 1) if (a, b) != (0, 0)]
BOTH = (1, -1)


def slot(a, b):
    return (a + 1) * 3 + (b + 1)


def kernel_values(target_x, target_y, source_x, source_y):
    dx = target_x - source_x
    dy = target_y - source_y
    square = dx * dx + dy * dy
    distance = square * lax.rsqrt(jnp.maximum(square, 1e-30))
    scaled = SCALE * distance
    clipped = jnp.minimum(distance, 1.0)
    left = 1.0 - clipped
    square = left * left
    return (1.0 + scaled) * jnp.exp(-scaled) * (square * square * (4.0 * clipped + 1.0))


def halves(value):
    high = value.astype(BF16)
    low = (value - high.astype(F32)).astype(BF16)
    return high, low


def packed(value):
    return jnp.concatenate(halves(value), axis=1)


def bf_dot(left, right):
    return jnp.dot(left, right, preferred_element_type=F32)


def split_dot(high, low, both):
    first = bf_dot(high, both)
    return first[:, :LANES] + first[:, LANES:] + bf_dot(low, both[:, :LANES])


def pick_dot(chosen, both):
    first = bf_dot(chosen, both)
    return first[:, :LANES] + first[:, LANES:]


def three_dot(left, right):
    (left_high, left_low), (right_high, right_low) = halves(left), halves(right)
    return bf_dot(left_high, right_high) + bf_dot(left_high, right_low) + bf_dot(left_low, right_high)


def full_dot(left, right, dims=((1,), (0,))):
    return lax.dot_general(left, right, (dims, ((), ())), precision=HIGH, preferred_element_type=F32)


def identity(size):
    row = lax.broadcasted_iota(jnp.int32, (size, size), 0)
    return (row == lax.broadcasted_iota(jnp.int32, (size, size), 1)).astype(F32)


def newton_inverse(matrix, result):
    size = matrix.shape[0]
    value = matrix[...]
    largest = jnp.max(jnp.sum(jnp.abs(value), axis=1, keepdims=True), axis=0, keepdims=True)
    alpha = 1.0 / largest
    least = LEAST_NOISE * alpha
    scale = 2.0 / (1.0 + least)
    first = scale * alpha
    result[...] = (2.0 * first) * identity(size) - (first * first) * value

    def step(dot, least):
        scale = 2.0 / (1.0 + least)
        current = result[...]
        product = dot(matrix[...], current)
        result[...] = scale * dot(current, 2.0 * identity(size) - scale * product)
        return 4.0 * least / ((1.0 + least) * (1.0 + least))

    least = lax.fori_loop(0, NEWTON_STEPS - 1, lambda _, least: step(three_dot, least),
                          4.0 * least / ((1.0 + least) * (1.0 + least)))
    step(full_dot, least)


def body(cfg, coords_ref, noise_ref, ids_ref, b_ref, x_ref, r_ref, *scratch):
    ref = dict(zip(cfg["names"], scratch))
    points, ov = cfg["points"], cfg["ov"]
    ext = points + ov
    gx, gy = cfg["gx"], cfg["gy"]
    seat, col = lax.axis_index("gx"), lax.axis_index("gy")
    mid = gy // 2

    def trades(r, c):
        return (c // mid + r) % 2

    def host(r, c):
        return (r + trades(r, c) * (2 - 4 * ((r // 2) % 2)), c)

    row, _ = host(seat, col)
    traded, kept = trades(seat, col) == 1, trades(seat, col) == 0
    has = {0: None, 1: col < gy - 1, -1: col > 0, "traded": traded}
    send_sem, recv_sem = ref["send"], ref["recv"]
    counter = [0]
    pending = {0: [], 1: [], -1: [], "traded": []}
    latest = []

    def guarded(which, action):
        if which == 0:
            action()
        else:
            pl.when(has[which])(action)

    def device(a, b):
        return host((row + a + gx) % gx, (col + b + gy) % gy)

    def heir(a, b):
        return host((seat + a + gx) % gx, (col + b + gy) % gy)

    def holder(a, b):
        return ((row + a + gx) % gx, (col + b + gy) % gy)

    mate = (seat + 2 - 4 * ((seat // 2) % 2), col)

    def copy_to(src, dst, target):
        key = counter[0]
        counter[0] += 1
        return pltpu.make_async_remote_copy(
            src_ref=src, dst_ref=dst, send_sem=send_sem.at[key], recv_sem=recv_sem.at[key],
            device_id=target, device_id_type=MESH)

    def send(src, dst, a, b, guard=None, target=None):
        out = b if guard is None else guard
        arrives = -b if guard is None else guard
        desc = copy_to(src, dst, device(a, b) if target is None else target)
        guarded(out, desc.start)
        pending[out].append(desc)
        latest.append((out, desc))
        return functools.partial(guarded, arrives, desc.wait_recv)

    def sent(begin, end):
        for out, desc in latest[begin:end]:
            guarded(out, desc.wait_send)
            pending[out][:] = [other for other in pending[out] if other is not desc]

    info_ref = ref["info"]
    info_ref[...] = jnp.concatenate([
        coords_ref[...], noise_ref[...],
        jnp.concatenate([ids_ref[...].astype(F32), jnp.zeros((1, points - ov), F32)], axis=1),
        jnp.zeros((4, points), F32)], axis=0)

    info_all = ref["info_all"]
    for n in range(9):
        if n != 4:
            info_all[n] = jnp.full(info_all.shape[1:], -1.0, F32)

    @pl.when(kept)
    def _():
        info_all[4] = info_ref[...]

    @pl.when((col == 0) | (col == gy - 1))
    def _():
        for name in ("ret", "halo", "part_in", "take_in", "give_in"):
            buf = ref[name]
            flat = math.prod(buf.shape[:-2])
            for n in range(flat):
                index, rest = [], n
                for d in reversed(buf.shape[:-2]):
                    index.append(rest % d)
                    rest //= d
                buf[tuple(reversed(index))] = jnp.zeros(buf.shape[-2:], F32)

    groups = cfg["groups"]

    def partner(group, offset):
        line, pair, core = seat // 4, (seat // 2) % 2, seat % 2
        if group == "plane":
            pair, other = (pair + offset % 2) % 2, (col + offset // 2) % gy
            return (4 * line + 2 * pair + core, other)
        core, line = (core + offset % 2) % 2, (line + offset // 2) % (gx // 4)
        return (4 * line + 2 * pair + core, col)

    barrier = pltpu.get_barrier_semaphore()
    for a, b in NEAR:
        for whom in (device, heir, holder):
            pl.semaphore_signal(barrier, inc=1, device_id=whom(a, b), device_id_type=MESH)
    pl.semaphore_signal(barrier, inc=1, device_id=mate, device_id_type=MESH)
    total = 3 * len(NEAR) + 1
    for group in groups:
        for offset in range(1, group[1]):
            pl.semaphore_signal(barrier, inc=1, device_id=partner(group[0], offset), device_id_type=MESH)
            total += 1
    pl.semaphore_wait(barrier, total)

    waits = [send(info_ref, info_all.at[slot(-a, -b)], a, b, target=heir(a, b)) for a, b in NEAR]
    waits.append(send(info_ref, info_all.at[4], 0, 0, guard="traded", target=mate))
    be = ref["be"]
    own = slice(0, points)

    def half(h):
        return slice(h * LANES, (h + 1) * LANES)

    came_right = [send(b_ref.at[:, half(h)], be.at[h, own], 0, 0, guard="traded", target=mate) for h in range(2)]

    @pl.when(kept)
    def _():
        for h in range(2):
            be[h, own] = b_ref[:, half(h)]

    for wait in waits:
        wait()

    gather, scatter = ref["gather"], ref["scatter"]

    def chosen_row(ids):
        sub = lax.broadcasted_iota(jnp.int32, (points, ov), 0).astype(F32)
        return (sub == ids).astype(F32).astype(BF16)

    def first_id(a, b):
        return float((3 * (1 - a) + (1 - b)) * points)

    def make_gather():
        for e, (a, b) in enumerate(NEAR):
            ids_col = jnp.transpose(info_all[slot(a, b), :, 0:ov])[:, 3:4] - first_id(a, b)
            lane = lax.broadcasted_iota(jnp.int32, (ov, points), 1).astype(F32)
            gather[e * ov:(e + 1) * ov, :] = (lane == ids_col).astype(F32).astype(BF16)

    def make_scatter():
        for e, (a, b) in enumerate(NEAR):
            scatter[:, e * ov:(e + 1) * ov] = chosen_row(info_all[slot(a, b), 3:4, 0:ov] - first_id(a, b))

    def borrow_first(k, h, own):
        out = ref["give_out"]
        asked = pick_dot(gather[...], packed(own))
        for e in range(8):
            a, b = NEAR[e]
            along, across = (a, b) if h == 0 else (b, a)
            out[k, h, slot(along, across)] = asked[e * ov:(e + 1) * ov]
        waits = []
        for step in BOTH:
            a, b = (step, 0) if h == 0 else (0, step)
            s = slot(step, -1)
            waits.append(send(out.at[k, h, s:s + 3], ref["take_in"].at[k, h, (1 - step) // 2], a, b))
        return waits

    def borrow_second(k, h, waits):
        for wait in waits:
            wait()
        out, came = ref["give_out"], ref["take_in"]
        waits = []
        for step in BOTH:
            mix = out.at[k, h, slot(0, step)]
            mix[...] = mix[...] + came[k, h, 0, step + 1] + came[k, h, 1, step + 1]
            a, b = (0, step) if h == 0 else (step, 0)
            waits.append(send(mix, ref["give_in"].at[k, h, (1 - step) // 2], a, b))
        return waits

    def borrow_end(k, h, waits):
        for wait in waits:
            wait()
        came, given = ref["take_in"], ref["give_in"]
        return came[k, h, 0, 1] + came[k, h, 1, 1] + given[k, h, 0] + given[k, h, 1]

    inverse = ref["inverse"]

    def precondition(k, extended, target, early=None, late=None):
        back, out = ref["ret"], ref["ret_out"]
        both, first = [], []
        for h in range(2):
            pack = ref["pack"].at[h]
            pack[...] = packed(extended[h])
            out[k, h] = split_dot(inverse[0, points:ext], inverse[1, points:ext], pack[...])
            waits = {}
            for a, b in ((0, 1), (0, -1), (1, 0), (-1, 0)):
                waits[a, b] = send(out.at[k, h], back.at[k, h, slot(-a, -b)], a, b)
            first.append(waits)

        def own_rows(h, carry):
            target[h] = split_dot(inverse[0, 0:points], inverse[1, 0:points], ref["pack"][h])
            return carry

        lax.fori_loop(0, 2, own_rows, 0)
        if early is not None:
            early()
        second = []
        for h in range(2):
            waits = []
            for step in BOTH:
                first[h][(0, step) if h == 0 else (step, 0)]()
            for step in BOTH:
                for other in BOTH:
                    if h == 0:
                        waits.append(send(back.at[k, h, slot(0, step)], back.at[k, h, slot(-other, step)],
                                          other, 0, guard=step))
                    else:
                        waits.append(send(back.at[k, h, slot(step, 0)], back.at[k, h, slot(step, -other)],
                                          0, other))
            for step in BOTH:
                waits.append(first[h][(step, 0) if h == 0 else (0, step)])
            second.append(waits)
        if late is not None:
            late()
        begin, leaving = len(latest), []
        for h in range(2):
            for wait in second[h]:
                wait()
            given = jnp.concatenate([packed(back[k, h, slot(a, b)]) for a, b in NEAR], axis=0)
            target[h] = target[h] + pick_dot(scatter[...], given)
            leaving.append([send(target.at[h], ref["halo"].at[k, h, (1 - step) // 2],
                                 *((step, 0) if h == 0 else (0, step))) for step in BOTH])
        return leaving, begin, len(latest)

    blocks = ref["blocks"]
    noise_col = ref["columns"]

    def operate(k, vector, target, started, hooks=(), early=None):
        halo, out, came = ref["halo"], ref["part_out"], ref["part_in"]
        waits, begin, end = started
        noise = noise_col[1, :, 2:3]
        for h in range(2):
            ref["pack"][h, own] = packed(vector[h])

        def from_here(n, carry):
            h, t = n // 3, n % 3
            out[k, h, t] = split_dot(blocks[h, 7 - 3 * t, 0], blocks[h, 7 - 3 * t, 1], ref["pack"][h, own])
            return carry

        lax.fori_loop(0, 6, from_here, 0)
        if early is not None:
            early()
        sources = ref["sources"]
        piece = points // 2

        def arrived(h, toward, rows):
            value = None
            for n, source in enumerate((-1, 1)):
                at = (toward + 1) * 3 + source + 1
                term = split_dot(blocks[h, at, 0, rows, :], blocks[h, at, 1, rows, :], sources[h, n])
                value = term if value is None else value + term
            return value

        def hand_on(h, rows):
            for toward in BOTH:
                part = out.at[k, h, 1 - toward, rows]
                part[...] = part[...] + arrived(h, toward, rows)
                a, b = (0, toward) if h == 0 else (toward, 0)
                later[h].append(send(part, came.at[k, h, (1 - toward) // 2, rows], a, b))

        later = [[], []]
        for h in range(2):
            for wait in waits[h]:
                wait()
            for n in range(2):
                sources[h, n] = packed(halo[k, h, n])
            hand_on(h, slice(0, piece))
        for h in range(2):
            hand_on(h, slice(piece, points))

        def own_sums(n, carry):
            h, rows = n // 2, pl.ds(pl.multiple_of(n % 2 * piece, piece), piece)
            out[k, h, 1, rows, :] = out[k, h, 1, rows, :] + arrived(h, 0, rows)
            return carry

        lax.fori_loop(0, 4, own_sums, 0)
        for hook in hooks:
            hook()
        for h in range(2):
            for wait in later[h]:
                wait()
            target[h] = (out[k, h, 1] + noise * vector[h]) + (came[k, h, 0] + came[k, h, 1])
        sent(begin, end)

    sums, gathered = ref["sums"], ref["gathered"]
    counts = [count for _, count in groups]
    offsets = [sum(counts[:g]) for g in range(len(groups))]
    open_waits = {}

    def reduce_start(k, stage):
        waits = []
        for offset in range(1, counts[stage]):
            desc = copy_to(sums.at[k, stage], gathered.at[k, offsets[stage] + offset],
                           partner(groups[stage][0], offset))
            desc.start()
            pending[0].append(desc)
            waits.append(desc.wait_recv)
        open_waits[k] = waits

    def reduce_end(k, stage):
        for wait in open_waits[k]:
            wait()
        value = sums[k, stage]
        for offset in range(1, counts[stage]):
            value = value + gathered[k, offsets[stage] + offset]
        sums[k, stage + 1] = value

    def reduce_open(k, pairs):
        rows = []
        for h in range(2):
            for left, right in pairs(h):
                rows.append(jnp.sum(left * right, axis=0, keepdims=True))
        rows.append(jnp.zeros((4, LANES), F32))
        sums[k, 0] = jnp.concatenate(rows, axis=0)
        reduce_start(k, 0)

    def reduce_next(k, stage):
        reduce_end(k, stage)
        if stage + 1 < len(groups):
            reduce_start(k, stage + 1)

    def reduced(k, h, which):
        return sums[k, len(groups), 2 * h + which:2 * h + which + 1, :]

    w0, n0, w1 = ref["w0"], ref["n0"], ref["w1"]
    z0, m0, m1, z1, n1 = ref["z0"], ref["m0"], ref["m1"], ref["z1"], ref["n1"]
    columns = ref["columns"]
    for b in (-1, 0, 1):
        columns[b + 1] = jnp.transpose(info_all[slot(0, b)])
    ids = info_all[4, 3:4, 0:ov]
    picked = jnp.zeros((32, ov), F32)
    line = lax.broadcasted_iota(jnp.int32, (8, points), 0)
    for a, b in NEAR:
        shift = jnp.where(line == 0, float(a), jnp.where(line == 1, float(b), 0.0))
        value = info_all[slot(a, b)] + shift
        high, middle = halves(value)
        low = (value - high.astype(F32) - middle.astype(F32)).astype(BF16)
        pieces = jnp.concatenate([high.astype(F32), middle.astype(F32), low.astype(F32), jnp.zeros((8, points), F32)])
        picked = picked + bf_dot(pieces.astype(BF16), chosen_row(ids - float(slot(a, b) * points)))
    picked = (picked[0:8] + picked[8:16]) + picked[16:24]
    wide = ref["wide"]
    wide[:, own] = info_all[4]
    wide[:, points:ext] = picked
    tall = ref["tall"]
    tall[...] = jnp.transpose(wide[...])
    matrix = ref["matrix"]

    def ext_rows(c, carry):
        rows = pl.ds(pl.multiple_of(c * LANES, LANES), LANES)
        value = kernel_values(tall[rows, 0:1], tall[rows, 1:2], wide[0:1, :], wide[1:2, :])
        at = lax.broadcasted_iota(jnp.int32, (LANES, ext), 0) + c * LANES
        diag = at == lax.broadcasted_iota(jnp.int32, (LANES, ext), 1)
        matrix[rows, :] = value + jnp.where(diag, wide[2:3, :], 0.0)
        return carry

    lax.fori_loop(0, ext // LANES, ext_rows, 0)

    def build(count, pair):
        def block_rows(n, carry):
            b, a = pair(n // (points // LANES))
            rows = pl.ds(pl.multiple_of(n % (points // LANES) * LANES, LANES), LANES)
            source = info_all[3 * a + 4]
            value = kernel_values(columns[b + 1, rows, 0:1], columns[b + 1, rows, 1:2],
                                  source[0:1, :] + a.astype(F32), source[1:2, :] - b.astype(F32))
            high, low = halves(value)
            blocks[0, slot(b, a), 0, rows, :] = high
            blocks[0, slot(b, a), 1, rows, :] = low
            high, low = halves(jnp.transpose(value))
            blocks[1, slot(a, b), 0, :, rows] = high
            blocks[1, slot(a, b), 1, :, rows] = low
            return carry

        lax.fori_loop(0, count * (points // LANES), block_rows, 0)

    full = ref["full"]
    at = 0
    for size in cfg["leaves"]:
        now = slice(at, at + size)
        before = slice(0, at)
        leaf, leaf_inverse = ref["leaf"].at[0:size, 0:size], ref["leaf_inverse"].at[0:size, 0:size]
        if at == 0:
            leaf[...] = matrix[now, now]
            newton_inverse(leaf, leaf_inverse)
        else:
            cross = matrix[before, now]
            reach = ref["reach"].at[0:at, 0:size]
            reach[...] = full_dot(full[before, before], cross)
            leaf[...] = matrix[now, now] - full_dot(matrix[now, before], reach[...])
            newton_inverse(leaf, leaf_inverse)
            moved = full_dot(reach[...], leaf_inverse[...])
            full[before, before] = full[before, before] + full_dot(moved, reach[...], ((1,), (1,)))
            full[before, now] = -moved
            full[now, before] = -full_dot(leaf_inverse[...], reach[...], ((1,), (1,)))
        if at == 0:
            make_gather()
            for wait in came_right:
                wait()
            waits = [borrow_first(0, h, be[h, own]) for h in range(2)]
        elif at + size == points:
            waits = [borrow_second(0, h, waits[h]) for h in range(2)]
        full[now, now] = leaf_inverse[...]
        at += size
    high, low = halves(full[...])
    inverse[0] = high
    inverse[1] = low

    for h in range(2):
        be[h, points:ext] = borrow_end(0, h, waits[h])

    started = precondition(0, be, z0, early=lambda: build(3, lambda n: (n - 1, 0 * n)),
                           late=lambda: (make_scatter(), build(2, lambda n: (0 * n, 2 * n - 1))))
    operate(0, z0, w0.at[:, own], started,
            early=lambda: build(4, lambda n: (2 * (n // 2) - 1, 2 * (n % 2) - 1)))

    def borrow(k, vector, between):
        waits = [borrow_first(k, h, vector[h, own]) for h in range(2)]
        between()
        waits = [borrow_second(k, h, waits[h]) for h in range(2)]
        for h in range(2):
            vector[h, points:ext] = borrow_end(k, h, waits[h])

    borrow(1, w0, lambda: reduce_open(0, lambda h: ((be[h, own], z0[h]), (z0[h], w0[h, own]))))
    started = precondition(1, w0, m0)
    reduce_next(0, 0)
    operate(1, m0, n0.at[:, own], started, [lambda: reduce_next(0, 1)])

    def first_step():
        for h in range(2):
            alpha = reduced(0, h, 0) / reduced(0, h, 1)
            z1[h] = z0[h] - alpha * m0[h]
            w1[h, own] = w0[h, own] - alpha * n0[h, own]
            be[h, own] = be[h, own] - alpha * w0[h, own]
        reduce_open(1, lambda h: ((be[h, own], z1[h]), (z1[h], w1[h, own])))

    borrow(2, n0, first_step)
    for h in range(2):
        alpha = reduced(0, h, 0) / reduced(0, h, 1)
        w1[h, points:ext] = w0[h, points:ext] - alpha * n0[h, points:ext]
    started = precondition(2, w1, m1)
    reduce_next(1, 0)

    def steps(h):
        gamma0, delta0 = reduced(0, h, 0), reduced(0, h, 1)
        gamma1, delta1 = reduced(1, h, 0), reduced(1, h, 1)
        alpha0 = gamma0 / delta0
        beta1 = gamma1 / gamma0
        alpha1 = gamma1 / (delta1 - beta1 * gamma1 / alpha0)
        return alpha0, beta1, alpha1, gamma1

    result, got = ref["result"], ref["got"]
    home = [[], []]

    def second_step():
        for h in range(2):
            alpha0, beta1, alpha1, _ = steps(h)
            direction = z1[h] + beta1 * z0[h]
            image = w1[h, own] + beta1 * w0[h, own]
            result[0, h] = alpha0 * z0[h] + alpha1 * direction
            be[h, own] = be[h, own] - alpha1 * image
            z1[h] = z1[h] - alpha1 * (m1[h] + beta1 * m0[h])
            w1[h, own] = w1[h, own] - (alpha1 * beta1) * n0[h, own]
            z0[h] = direction
            w0[h, own] = image
            for n, piece in enumerate((result.at[0, h], z1.at[h], z0.at[h])):
                home[h].append(send(piece, got.at[n, h], 0, 0, guard="traded", target=mate))

    operate(2, m1, n1, started, [lambda: reduce_next(1, 1), second_step])
    for h in range(2):
        w1[h, own] = w1[h, own] - steps(h)[2] * n1[h]
    reduce_open(2, lambda h: ((be[h, own], z1[h]), (z1[h], w1[h, own])))
    for stage in range(len(groups)):
        reduce_next(2, stage)
    for h in range(2):
        _, _, alpha1, gamma1 = steps(h)
        gamma2, delta2 = reduced(2, h, 0), reduced(2, h, 1)
        beta2 = gamma2 / gamma1
        alpha2 = gamma2 / (delta2 - beta2 * gamma2 / alpha1)
        result[1, h] = be[h, own] - alpha2 * (w1[h, own] + beta2 * w0[h, own])
        last = send(result.at[1, h], got.at[3, h], 0, 0, guard="traded", target=mate)

        @pl.when(kept)
        def _():
            x_ref[:, half(h)] = result[0, h] + alpha2 * (z1[h] + beta2 * z0[h])
            r_ref[:, half(h)] = result[1, h]

        for wait in home[h]:
            wait()

        @pl.when(traded)
        def _():
            x_ref[:, half(h)] = got[0, h] + alpha2 * (got[1, h] + beta2 * got[2, h])

        home[h] = last
    for h in range(2):
        home[h]()

        @pl.when(traded)
        def _():
            r_ref[:, half(h)] = got[3, h]

    for which in (0, 1, -1, "traded"):
        def drain(descs=pending[which]):
            for desc in descs:
                desc.wait_send()
        guarded(which, drain)
    assert counter[0] <= cfg["copies"], counter[0]


def make(gx, gy, points, ov, rhs):
    ext = points + ov
    groups = (("plane", 2 * gy), ("line", gx // 2))
    each = [count for _, count in groups]
    copies = 8 + 3 + 8 + 3 * (16 + 12 + 8) + 3 * sum(n - 1 for n in each)
    stages = len(groups)
    half = (2, points, LANES)
    tall = (2, ext, LANES)
    shapes = {
        "send": pltpu.SemaphoreType.DMA((copies,)),
        "recv": pltpu.SemaphoreType.DMA((copies,)),
        "info": ((8, points), F32),
        "info_all": ((9, 8, points), F32),
        "gather": ((8 * ov, points), BF16),
        "scatter": ((points, 8 * ov), BF16),
        "ret": ((3, 2, 9, ov, LANES), F32),
        "ret_out": ((3, 2, ov, LANES), F32),
        "halo": ((3, 2, 2, points, LANES), F32),
        "part_out": ((3, 2, 3, points, LANES), F32),
        "part_in": ((3, 2, 2, points, LANES), F32),
        "give_out": ((3, 2, 9, ov, LANES), F32),
        "take_in": ((3, 2, 2, 3, ov, LANES), F32),
        "give_in": ((3, 2, 2, ov, LANES), F32),
        "pack": ((2, ext, 2 * LANES), BF16),
        "inverse": ((2, ext, ext), BF16),
        "blocks": ((2, 9, 2, points, points), BF16),
        "sources": ((2, 2, points, 2 * LANES), BF16),
        "columns": ((3, points, 8), F32),
        "wide": ((8, ext), F32),
        "tall": ((ext, 8), F32),
        "matrix": ((ext, ext), F32),
        "full": ((ext, ext), F32),
        "leaf": ((256, 256), F32),
        "leaf_inverse": ((256, 256), F32),
        "reach": ((points, 256), F32),
        "result": ((2, 2, points, LANES), F32),
        "got": ((4, 2, points, LANES), F32),
        "sums": ((3, stages + 1, 8, LANES), F32),
        "gathered": ((3, sum(each), 8, LANES), F32),
        "be": (tall, F32), "w0": (tall, F32), "n0": (tall, F32), "w1": (tall, F32),
        "z0": (half, F32), "m0": (half, F32), "m1": (half, F32), "z1": (half, F32), "n1": (half, F32),
    }
    cfg = {"names": tuple(shapes), "points": points, "ov": ov, "gx": gx, "gy": gy, "groups": groups,
           "copies": copies, "leaves": (256,) * (points // 256) + (ov,)}
    scratch = [pltpu.VMEM(*v) if isinstance(v, tuple) else v for v in shapes.values()]
    whole = pl.BlockSpec(memory_space=pltpu.VMEM)
    call = pl.pallas_call(
        functools.partial(body, cfg),
        out_shape=(jax.ShapeDtypeStruct((points, rhs), F32),) * 2,
        in_specs=[whole] * 4,
        out_specs=(whole, whole),
        scratch_shapes=scratch,
        compiler_params=pltpu.CompilerParams(
            collective_id=0, has_side_effects=True, vmem_limit_bytes=67043328),
    )

    def shards(right_side, coords, noise, intersect):
        x, r = call(coords.reshape(2, points), noise.reshape(1, points), intersect.reshape(1, ov),
                    right_side.reshape(points, rhs))
        return x.reshape(right_side.shape), r.reshape(right_side.shape)

    return shards


def solution(mesh):
    gx, gy = mesh.shape["gx"], mesh.shape["gy"]

    def run(right_side, coords, noise, intersect):
        points, rhs = right_side.shape[2:]
        spec4, spec3 = P("gx", "gy", None, None), P("gx", "gy", None)
        return jax.shard_map(
            make(gx, gy, points, intersect.shape[2], rhs), mesh=mesh,
            in_specs=(spec4, spec4, spec3, spec3), out_specs=(spec4, spec4), check_vma=False,
        )(right_side, coords, noise, intersect)

    return run
```
